32 devices in a mesh: groups: 2 (over y), fsdp: 4 (over z), mp: 2 (over x), sub: 2 (over core).
Axes of the slice: x: 2, y: 2, z: 4, core: 2. Of those that a mesh axis runs over, the one named last changes fastest.
Arguments:
- hidden: bfloat16 [128, 36864], P(('groups', 'fsdp', 'sub'), 'mp'), parts along dimension 0, may hold values from -6 to 6
- residual: bfloat16 [128, 4608], P(('groups', 'fsdp', 'sub')), parts along dimension 0, may hold values from -6 to 6
- down_packed: int32 [4608, 4608], P('mp', 'fsdp'), may hold values from -2147483648 to 2147483646
- down_scale: bfloat16 [288, 4608], P('mp', 'fsdp'), may hold values from 0.00049972534 to 0.0019989014
- post_gain: float32 [4608], replicated, may hold values from 0.1 to 1.9
- final_gain: float32 [4608], replicated, may hold values from 0.1 to 1.9
- embed_packed: int32 [8192, 576], P(('fsdp', 'mp', 'sub')), may hold values from -2147483648 to 2147483646
- embed_scale: bfloat16 [8192, 36], P(('fsdp', 'mp', 'sub')), may hold values from 0.0059814453 to 0.029907227
- targets: int32 [128], P(('groups', 'fsdp', 'sub')), parts along dimension 0, may hold values from 0 to 8191
- loss_mask: int32 [128], P(('groups', 'fsdp', 'sub')), parts along dimension 0, may hold values 0 or 1
Outputs:
- token_loss: float32 [128], P(('groups', 'fsdp', 'sub')), parts along dimension 0
- mean_loss: float32 [2], P('groups'), parts along dimension 0
The draws below stay inside these ranges and needn't reach their ends.
There are 2 independent parts, one for each index of `groups`. The reference program is written for one: setup_inputs(seed, part) draws one part's arguments, and reference() takes and returns one part's arrays. A program takes and returns all parts, laid end to end along the dimension named above; an argument that names none is the same for every part. Nothing has to cross between parts.
Inputs may be any that keep to these rules, and one draw needn't show every extreme that they name: `down_packed`: bits 4 k to 4 k + 3 of the word in row r hold the signed code of row 8 r + k of the down projection, k = 0..7. `embed_packed`: bits 4 k to 4 k + 3 of the word in column j hold the signed code of column k * 576 + j of the embedding, k = 0..7.
All inputs are finite; a program needn't handle non-finite values. No bound on the sum of `loss_mask` on one device may be relied on, other than what follows from the above.
Results may differ from the reference program's by a relative error of at most 0.00097.
Values may be sent and summed in bfloat16 or wider, within the bound.
A program may use at most 128 MiB of HBM per device.

```python
import math
import jax
import jax.numpy as jnp
from jax import lax

D = 4608
FF = 36864
GROUP = 128
VOCAB = 8192
TOKENS = 64
N_MP = 2


def with_ends(entries, stream_key, smallest, largest):
    shape = entries.shape
    spot = [jax.random.randint(jax.random.fold_in(stream_key, axis), (), 0, shape[axis]) for axis in range(len(shape))]
    entries = entries.at[tuple(spot)].set(smallest)
    longest = shape.index(max(shape))
    spot[longest] = (spot[longest] + 1) % shape[longest]
    return entries.at[tuple(spot)].set(largest)


def levels(own_key, extent, pieces, smallest, top_value):
    gain, own = 1.0, jax.random.fold_in(own_key, 6)
    for dim, blocks in pieces:
        steps = jnp.exp(jax.random.uniform(jax.random.fold_in(own, dim), (blocks,), jnp.float32, smallest / len(pieces), top_value / len(pieces)))
        gain = gain * jnp.repeat(steps, extent[dim] // blocks).reshape([-1 if axis == dim else 1 for axis in range(len(extent))])
    return gain


def scatter_about(rng, extent, scale, reach, shards=(), held_as=jnp.bfloat16):
    gain = levels(rng, extent, shards, -0.22, 0.18) if shards else 1.0
    drawn = jax.random.normal(rng, extent, jnp.float32) * scale * gain
    return jnp.minimum(jnp.maximum(drawn, -reach), reach).astype(held_as)


def setup_inputs(seed: int = 0, part: int = 0) -> dict:
    streams_of = jax.random.split(jax.random.key(seed), 11)
    part_keys = jax.random.split(jax.random.fold_in(streams_of[10], part), 11)
    return {
        "hidden": scatter_about(part_keys[0], (TOKENS, FF), 1.0, 6.0, ((0, 8), (1, 2))),
        "residual": scatter_about(part_keys[1], (TOKENS, D), 1.0, 6.0, ((0, 8),)),
        "down_packed": with_ends(jax.random.randint(streams_of[2], (FF // 8, D), -2147483648, 2147483647), jax.random.fold_in(streams_of[2], 1), -2147483648, 2147483646).astype(jnp.int32),
        "down_scale": jnp.clip(jnp.exp(math.log(0.0019989014) - 1.3862944 * jax.random.uniform(streams_of[3], (FF // GROUP, D), jnp.float32) ** levels(streams_of[3], (FF // GROUP, D), ((0, 2), (1, 4)), -0.2, 0.2)), 0.00049972534, 0.0019989014).astype(jnp.bfloat16),
        "post_gain": jnp.clip(1.0 + 0.18 * jax.random.normal(streams_of[4], (D,), jnp.float32), 0.1, 1.9),
        "final_gain": jnp.clip(1.0 + 0.18 * jax.random.normal(streams_of[5], (D,), jnp.float32), 0.1, 1.9),
        "embed_packed": with_ends(jax.random.randint(streams_of[6], (VOCAB, D // 8), -2147483648, 2147483647), jax.random.fold_in(streams_of[6], 1), -2147483648, 2147483646).astype(jnp.int32),
        "embed_scale": jnp.clip(jnp.exp(math.log(0.029907227) - 1.609438 * jax.random.uniform(streams_of[7], (VOCAB, D // GROUP), jnp.float32) ** levels(streams_of[7], (VOCAB, D // GROUP), ((0, 16),), -0.2, 0.2)), 0.0059814453, 0.029907227).astype(jnp.bfloat16),
        "targets": with_ends(jax.random.randint(part_keys[8], (TOKENS,), 0, VOCAB), jax.random.fold_in(part_keys[8], 1), 0, VOCAB - 1).astype(jnp.int32),
        "loss_mask": with_ends((jax.random.randint(part_keys[9], (TOKENS,), 0, 4) < 3).astype(jnp.int32), jax.random.fold_in(part_keys[9], 1), 0, 1),
    }


EPS = 1e-06
CAP = 30.0

def signed_planes(words):
    shifts = (28 - 4 * jnp.arange(8, dtype=jnp.int32))[None, :, None]
    lifted = jnp.left_shift(words[:, None, :], shifts)
    return jnp.right_shift(lifted, 28)

def dequant_down(words, scales):
    cols = words.shape[1]
    codes = signed_planes(words).astype(jnp.bfloat16)
    grouped = codes.reshape(scales.shape[0], -1, cols) * scales[:, None, :]
    return grouped.reshape(-1, cols)

def dequant_embed(words, scales):
    rows = words.shape[0]
    codes = signed_planes(words).astype(jnp.bfloat16)
    grouped = codes.reshape(rows, scales.shape[1], -1) * scales[:, :, None]
    return grouped.reshape(rows, -1)

def reference(hidden, residual, down_packed, down_scale, post_gain, final_gain, embed_packed, embed_scale, targets, loss_mask):
    block = FF // N_MP
    ffn = jnp.zeros((TOKENS, D), jnp.float32)
    for b in range(N_MP):
        weight = dequant_down(down_packed[b * block // 8:(b + 1) * block // 8], down_scale[b * block // GROUP:(b + 1) * block // GROUP])
        ffn = ffn + jnp.dot(hidden[:, b * block:(b + 1) * block], weight, preferred_element_type=jnp.float32)
    normed = ffn * lax.rsqrt(lax.optimization_barrier(jnp.mean(ffn * ffn, axis=-1, keepdims=True)) + EPS) * post_gain
    stream = residual.astype(jnp.float32) + normed
    states = (stream * lax.rsqrt(lax.optimization_barrier(jnp.mean(stream * stream, axis=-1, keepdims=True)) + EPS) * final_gain).astype(jnp.bfloat16)
    vrows = VOCAB // N_MP
    exp_sums = jnp.zeros((TOKENS,), jnp.float32)
    target_logits = jnp.zeros((TOKENS,), jnp.float32)
    for b in range(N_MP):
        embed = dequant_embed(embed_packed[b * vrows:(b + 1) * vrows], embed_scale[b * vrows:(b + 1) * vrows])
        logits = lax.dot_general(states, embed, (((1,), (1,)), ((), ())), preferred_element_type=jnp.float32)
        capped = CAP * jnp.tanh(logits / CAP)
        exp_sums = exp_sums + lax.optimization_barrier(jnp.sum(jnp.exp(capped), axis=1))
        ids = b * vrows + jnp.arange(vrows, dtype=jnp.int32)
        hits = targets[:, None] == ids[None, :]
        target_logits = target_logits + lax.optimization_barrier(jnp.sum(jnp.where(hits, capped, 0.0), axis=1))
    weights = loss_mask.astype(jnp.float32)
    token_loss = weights * (jnp.log(exp_sums) - target_logits)
    mean_loss = jnp.sum(token_loss) / jnp.maximum(jnp.sum(weights), 1.0)
    return (token_loss, mean_loss.reshape(1))
```

```python
import functools

import jax
import jax.numpy as jnp
from jax import lax
from jax.experimental import pallas as pl
from jax.experimental.pallas import tpu as pltpu
from jax.sharding import PartitionSpec as P

EPS = 1e-06
CAP = 30.0
MESH = pl.DeviceIdType.MESH
PLANES = 8
GROUP = 128
PIECES = (9, 8, 6, 4, 3, 2, 1)


def remote(src, dst, send, recv, f, m, s):
    return pltpu.make_async_remote_copy(
        src_ref=src,
        dst_ref=dst,
        send_sem=send,
        recv_sem=recv,
        device_id={"fsdp": f, "mp": m, "sub": s},
        device_id_type=MESH,
    )


def mark(name):
    pass


def kernel(
    nf, nm, hidden_hbm, residual_hbm, words_hbm, scale_hbm, post_hbm, final_hbm, embed_hbm, embed_scale_hbm,
    targets_hbm, mask_hbm,
    out,
    hidden, residual, words, scale, post_gain, final_gain, embed_words, embed_scale, targets, mask,
    scale_f, embed_f, post_z, final_z, weight, embed, perm, sorted_own, gathered,
    near_own, near_in, near_part, near_mid, far_own, far_in, far_part, far_mid,
    ffn, res, states, moments, moment, info, infos, sums,
    local_sem, hid_send, hid_recv, pair_sem, near_sem, far_sem, near_mp, far_mp, res_sem, info_sem,
    near_send, near_recv, far_send, far_recv, near_fwd, far_fwd, mom_sem, sum_sem,
):
    f, m, s = lax.axis_index("fsdp"), lax.axis_index("mp"), lax.axis_index("sub")
    n = nf * nm * 2
    me = (f * nm + m) * 2 + s
    tok = hidden.shape[0]
    half_rows, cols = words.shape
    half_k = half_rows * PLANES
    total = tok * 2 * nf
    width_d = nf * cols
    pieces, piece = gathered.shape[1], gathered.shape[4]
    groups = half_k // GROUP
    per = GROUP // PLANES
    rest = nf - 1
    low = f < nf - nf // 2
    far = jnp.where(low, nf - 1, 0)
    first = jnp.where(low, 0, 1)
    up, down = lax.rem(f + 1, nf), lax.rem(f + nf - 1, nf)
    has_up, has_down = f < nf - 1, f > 0
    inner = jnp.logical_and(has_up, has_down)

    def where_is(q):
        return q // (2 * nm), (q // 2) % nm, q % 2

    barrier = pltpu.get_barrier_semaphore()

    def greet(pf, pm, ps):
        pl.semaphore_signal(
            barrier, inc=1, device_id={"fsdp": pf, "mp": pm, "sub": ps}, device_id_type=MESH
        )

    @pl.when(has_up)
    def _():
        greet(up, m, 0)
        greet(up, m, 1)

    @pl.when(has_down)
    def _():
        greet(down, m, 0)
        greet(down, m, 1)

    greet(f, m, 1 - s)
    for d in range(1, nm):
        greet(f, lax.rem(m + d, nm), s)

    def load(i, src, dst):
        copy = pltpu.make_async_copy(src, dst, local_sem.at[i])
        copy.start()
        return copy

    load_hidden = load(0, hidden_hbm, hidden)
    load_words = load(
        1, words_hbm.at[pl.ds(pl.multiple_of(s * half_rows, 8), half_rows)], words
    )
    load_scale = load(2, scale_hbm, scale)
    loads = [
        load(3, embed_hbm, embed_words), load(4, embed_scale_hbm, embed_scale),
        load(5, residual_hbm, residual), load(6, post_hbm, post_gain), load(7, final_hbm, final_gain),
        load(8, targets_hbm, targets), load(9, mask_hbm, mask),
    ]

    width = perm.shape[0]
    row = lax.broadcasted_iota(jnp.int32, (width, width), 0)
    col = lax.broadcasted_iota(jnp.int32, (width, width), 1)
    inside = jnp.bitwise_and(col, GROUP - 1)
    source = (col - inside) + jnp.bitwise_and(inside, per - 1) * PLANES + jnp.right_shift(inside, 4)
    perm[...] = jnp.where(row == source, 1.0, 0.0).astype(jnp.bfloat16)

    mark("hidden_wait")
    load_hidden.wait()
    mark("permute")
    own = hidden[...].astype(jnp.float32)
    spans = 2 * half_k // width
    stacked = jnp.concatenate(
        [own[:, c * width:(c + 1) * width] for c in range(spans)], axis=0
    ).astype(jnp.bfloat16)
    ordered = jnp.dot(stacked, perm[...], preferred_element_type=jnp.float32)
    for c in range(spans):
        h, at = c * width // half_k, c * width % half_k
        sorted_own[h, at // piece, :, at % piece:at % piece + width] = ordered[
            c * tok:(c + 1) * tok
        ].astype(jnp.bfloat16)

    mark("barrier")
    count = 1 + (nm - 1) + 2 * has_up.astype(jnp.int32) + 2 * has_down.astype(jnp.int32)
    pl.semaphore_wait(barrier, count)
    mark("send1")

    def first_hop(way, i):
        target = up if way == 0 else down
        for h in (0, 1):
            remote(
                sorted_own.at[h, i], gathered.at[f, i, s], hid_send.at[way, 0], hid_recv.at[f, i],
                target, m, h,
            ).start()

    def block_at(way, j):
        return lax.rem(f - j + nf, nf) if way == 0 else lax.rem(f + j, nf)

    def held(way, j):
        return f >= j if way == 0 else f + j <= nf - 1

    def arrive(b, i):
        remote(
            gathered.at[b, i], gathered.at[b, i], hid_send.at[0, 0], hid_recv.at[b, i], f, m, 1 - s
        ).wait_recv()

    def pass_on(j, i):
        for way in (0, 1):
            b = block_at(way, j)
            target = up if way == 0 else down

            @pl.when(jnp.logical_and(inner, held(way, j)))
            def _():
                arrive(b, i)
                remote(
                    gathered.at[b, i], gathered.at[b, i], hid_send.at[way, j], hid_recv.at[b, i],
                    target, m, s,
                ).start()

    for i in range(pieces):
        @pl.when(has_up)
        def _():
            first_hop(0, i)

        @pl.when(has_down)
        def _():
            first_hop(1, i)

    swap = remote(
        sorted_own.at[1 - s], gathered.at[f, :, s], pair_sem.at[0], pair_sem.at[1], f, m, 1 - s
    )
    swap.start()
    gathered[f, :, s] = sorted_own[s]

    mark("deq")
    load_scale.wait()
    scale_f[...] = scale[...].astype(jnp.float32)
    load_words.wait()

    def dequant(g, carry):
        w = words[pl.ds(pl.multiple_of(g * per, per), per), :]
        sc = scale_f[pl.ds(s * groups + g, 1), :]
        for k in range(PLANES):
            code = jnp.right_shift(jnp.left_shift(w, 28 - 4 * k), 28) if k < 7 else jnp.right_shift(w, 28)
            weight[pl.ds(pl.multiple_of(g * GROUP + k * per, per), per), :] = (
                code.astype(jnp.float32) * sc
            ).astype(jnp.bfloat16)
        return carry

    each = groups // pieces
    lag = min(3, pieces)
    for i in range(pieces):
        lax.fori_loop(i * each, (i + 1) * each, dequant, 0)
        if i >= lag and nf > 2:
            pass_on(1, i - lag)

    mark("deqE")
    for copy in loads:
        copy.wait()
    embed_f[...] = embed_scale[...].astype(jnp.float32)
    packed, vocab = embed_words.shape
    span = packed * PLANES // embed_f.shape[0]
    step = 32
    blocks = packed // step

    def dequant_embed(i, carry):
        w = embed_words[pl.ds(pl.multiple_of(i * step, step), step), :]
        for k in range(PLANES):
            code = jnp.right_shift(jnp.left_shift(w, 28 - 4 * k), 28) if k < 7 else jnp.right_shift(w, 28)
            sc = embed_f[pl.ds((k * packed + i * step) // span, 1), :]
            embed[pl.ds(pl.multiple_of(k * packed + i * step, step), step), :] = (
                code.astype(jnp.float32) * sc
            ).astype(jnp.bfloat16)
        return carry

    def dequant_some(part, parts):
        lax.fori_loop(part * blocks // parts, (part + 1) * blocks // parts, dequant_embed, 0)

    for part in range(lag):
        dequant_some(part, lag)
        if nf > 2:
            pass_on(1, pieces - lag + part)
    for j in range(2, nf - 2):
        for i in range(pieces):
            pass_on(j, i)

    mark("prep")
    post_row, final_row = post_gain[...].reshape(1, width_d), final_gain[...].reshape(1, width_d)
    own_res = residual[...].astype(jnp.float32)
    for z in range(nf):
        post_z[z] = post_row[:, z * cols:(z + 1) * cols]
        final_z[z] = final_row[:, z * cols:(z + 1) * cols]
        res[s, f, z] = own_res[:, z * cols:(z + 1) * cols].astype(jnp.bfloat16)
    token = lax.broadcasted_iota(jnp.int32, (tok, 128), 0)
    side = lax.broadcasted_iota(jnp.int32, (tok, 128), 1)
    entry = jnp.zeros((tok, 128), jnp.int32)
    for i in range(tok):
        entry = jnp.where(token == i, jnp.where(side < 64, targets[i], mask[i]), entry)
    info[...] = entry
    infos[me] = entry

    mark("near_mm")
    swap.wait_recv()
    edge = jnp.logical_not(inner)
    near_acc = jnp.zeros((rest * 2 * tok, cols), jnp.float32)
    for i in range(pieces):
        if nf > 3:
            pass_on(nf - 2, i)
        for b in range(nf):
            @pl.when(jnp.logical_and(edge, jnp.logical_and(f != b, far != b)))
            def _():
                arrive(b, i)

        lhs = gathered[pl.ds(first, rest), i].astype(jnp.float32).reshape(
            rest * 2 * tok, piece
        ).astype(jnp.bfloat16)
        near_acc = near_acc + jnp.dot(
            lhs, weight[i * piece:(i + 1) * piece], preferred_element_type=jnp.float32
        )
    for b in range(rest):
        for h in (0, 1):
            at = (2 * b + h) * tok
            near_own[h, b * tok:(b + 1) * tok] = near_acc[at:at + tok]
    near_swap = remote(
        near_own.at[1 - s], near_in, near_sem.at[0], near_sem.at[1], f, m, 1 - s
    )
    near_swap.start()

    def to_peers(part, mid, sems):
        for d in range(1, nm):
            remote(
                part, mid.at[m], sems.at[0], sems.at[1], f, lax.rem(m + d, nm), s
            ).start()

    def peers(mid, sems):
        ref = mid.at[pl.ds(0, nm - 1)]
        return remote(ref, ref, sems.at[0], sems.at[1], f, m, 1 - s)

    def gather_peers(part, mid, sems):
        if nm > 1:
            peers(mid, sems).wait_recv()
        full = part[...]
        for d in range(1, nm):
            full = full + mid[lax.rem(m + d, nm)]
        return full

    def to_columns(src, dst, sems, recv):
        for d in range(1, nf):
            remote(src, dst, sems, recv, lax.rem(f + d, nf), m, s).start()

    def early_sends():
        to_columns(res.at[s, f], res.at[s, f], res_sem.at[0], res_sem.at[1])
        for d in range(1, n):
            pf, pm, ps = where_is(lax.rem(me + d, n))
            remote(info, infos.at[me], info_sem.at[0], info_sem.at[1], pf, pm, ps).start()

    mark("far_mm")
    far_acc = jnp.zeros((2 * tok, cols), jnp.float32)
    reduce_at, send_at = min(2, pieces - 1), min(6, pieces - 1)
    for i in range(pieces):
        @pl.when(edge)
        def _():
            arrive(far, i)

        lhs = gathered[far, i].astype(jnp.float32).reshape(2 * tok, piece).astype(jnp.bfloat16)
        far_acc = far_acc + jnp.dot(
            lhs, weight[i * piece:(i + 1) * piece], preferred_element_type=jnp.float32
        )
        if i == reduce_at:
            near_swap.wait_recv()
            near_part[...] = near_own[s] + near_in[...]
            to_peers(near_part, near_mid, near_mp)
        if i == send_at:
            early_sends()
    for h in (0, 1):
        far_own[h] = far_acc[h * tok:(h + 1) * tok]
    mark("far_swap")
    far_swap = remote(far_own.at[1 - s], far_in, far_sem.at[0], far_sem.at[1], f, m, 1 - s)
    far_swap.start()

    near_ffn = gather_peers(near_part, near_mid, near_mp)
    ffn[pl.ds(first, rest)] = near_ffn.reshape(rest, tok, cols)
    gains = post_z[f] * final_z[f]
    near_at = pl.ds(first, rest)
    states[f, s, near_at] = (near_ffn * gains).reshape(rest, tok, cols).astype(jnp.bfloat16)

    def near_to(z, pf, ps, send, recv):
        return remote(
            states.at[z, s, near_at], states.at[z, s, near_at], send, recv, pf, m, ps
        )

    def near_span(z):
        return pl.ds(jnp.where(z < nf - nf // 2, 0, 1), rest)

    def far_spot(z):
        return jnp.where(z < nf - nf // 2, nf - 1, 0)

    for d in range(1, nf):
        near_to(f, lax.rem(f + d, nf), s, near_send, near_recv.at[f]).start()
    near_to(f, f, 1 - s, near_fwd.at[nf], near_fwd.at[f]).start()

    mark("far_in")
    far_swap.wait_recv()
    far_part[...] = far_own[s] + far_in[...]
    to_peers(far_part, far_mid, far_mp)
    mark("far_mp")
    far_ffn = gather_peers(far_part, far_mid, far_mp)
    ffn[far] = far_ffn
    states[f, s, far] = (far_ffn * gains).astype(jnp.bfloat16)

    def far_to(z, pf, ps, send, recv):
        spot = far_spot(z)
        return remote(states.at[z, s, spot], states.at[z, s, spot], send, recv, pf, m, ps)

    for d in range(1, nf):
        far_to(f, lax.rem(f + d, nf), s, far_send, far_recv.at[f]).start()
    far_to(f, f, 1 - s, far_fwd.at[nf], far_fwd.at[f]).start()

    mark("res_wait")
    res_all = res.at[s, pl.ds(0, rest)]
    res_in = remote(res_all, res_all, res_sem.at[0], res_sem.at[1], f, m, 1 - s)
    res_in.wait_recv()
    res_swap = remote(res.at[s], res.at[s], res_sem.at[2], res_sem.at[3], f, m, 1 - s)
    res_swap.start()
    mark("moments")
    mine = nf * tok
    y = ffn[...].reshape(mine, cols)
    r = res[s, :, f].astype(jnp.float32).reshape(mine, cols)
    g = y * post_z[f]
    lane = lax.broadcasted_iota(jnp.int32, (mine, 128), 1)

    def row_sum(v):
        return jnp.sum(v, axis=1, keepdims=True)

    moments[f] = jnp.where(
        lane < 64,
        jnp.where(lane < 32, row_sum(y * y), row_sum(r * r)),
        jnp.where(lane < 96, row_sum(r * g), row_sum(g * g)),
    )
    to_columns(moments.at[f], moments.at[f], mom_sem.at[0], mom_sem.at[1])

    mark("near_fwd")

    def nearer(d):
        return jnp.where(low, lax.rem(f + d, nf), lax.rem(f + nf - d, nf))

    def same(z, span, sems, recv):
        ref = states.at[z, s, span]
        return remote(ref, ref, sems, recv, f, m, 1 - s)

    def other(z, span, sems, recv):
        ref = states.at[z, 1 - s, span]
        return remote(ref, ref, sems, recv, f, m, 1 - s)

    for d in range(1, nf):
        z = nearer(d)
        same(z, near_span(z), near_send, near_recv.at[z]).wait_recv()
        same(z, near_span(z), near_fwd.at[nf], near_fwd.at[z]).start()

    mark("logits0")
    res_other = res.at[1 - s]
    remote(res_other, res_other, res_sem.at[2], res_sem.at[3], f, m, 1 - s).wait_recv()
    base = jnp.zeros((2 * total, vocab), jnp.float32)
    for z in range(nf):
        rf = res[:, :, z].astype(jnp.float32).reshape(total, cols) * final_z[z]
        high = rf.astype(jnp.bfloat16)
        rest_of = (rf - high.astype(jnp.float32)).astype(jnp.bfloat16)
        base = base + jnp.dot(
            jnp.concatenate([high, rest_of], axis=0), embed[z * cols:(z + 1) * cols],
            preferred_element_type=jnp.float32,
        )
    base = base[0:total] + base[total:]

    mark("info")
    info_all = infos.at[pl.ds(0, n - 1)]
    info_in = remote(info_all, info_all, info_sem.at[0], info_sem.at[1], f, m, 1 - s)
    info_in.wait_recv()
    rows = jnp.concatenate(
        [infos[b * nm * 2 + h] for h in (0, 1) for b in range(nf)], axis=0
    )
    counted = jnp.broadcast_to(rows[:, 64:65].astype(jnp.float32), (total, 128))
    weights = jnp.transpose(
        jnp.concatenate([counted, jnp.zeros((total, 128), jnp.float32)], axis=0)
    )[0:1, :]

    mark("far_fwd")
    for d in range(1, nf):
        z = nearer(d)
        same(z, far_spot(z), far_send, far_recv.at[z]).wait_recv()
        same(z, far_spot(z), far_fwd.at[nf], far_fwd.at[z]).start()

    mark("moments_in")
    mom_all = moments.at[pl.ds(0, rest)]
    mom_in = remote(mom_all, mom_all, mom_sem.at[0], mom_sem.at[1], f, m, 1 - s)
    mom_in.wait_recv()
    moment[s] = jnp.sum(moments[...], axis=0)
    mom_swap = remote(moment.at[s], moment.at[s], mom_sem.at[2], mom_sem.at[3], f, m, 1 - s)
    mom_swap.start()

    mark("logits1")
    main = jnp.zeros((total, vocab), jnp.float32)
    for d in range(nf):
        z = nearer(d)
        other(z, near_span(z), near_fwd.at[nf], near_fwd.at[z]).wait_recv()
        other(z, far_spot(z), far_fwd.at[nf], far_fwd.at[z]).wait_recv()
        lhs = states[z].astype(jnp.float32).reshape(total, cols).astype(jnp.bfloat16)
        main = main + jnp.dot(
            lhs, embed[pl.ds(pl.multiple_of(z * cols, 32), cols), :], preferred_element_type=jnp.float32
        )
    moment_other = moment.at[1 - s]
    remote(
        moment_other, moment_other, mom_sem.at[2], mom_sem.at[3], f, m, 1 - s
    ).wait_recv()
    both_mom = moment[...].reshape(total, 128)
    inv = lax.rsqrt(both_mom[:, 0:1] / width_d + EPS)
    square = both_mom[:, 32:33] + inv * (2.0 * both_mom[:, 64:65] + inv * both_mom[:, 96:97])
    inv2 = lax.rsqrt(square / width_d + EPS)
    logits = (base + main * inv) * inv2
    capped = CAP * jnp.tanh(logits / CAP)
    ids = me * vocab + lax.broadcasted_iota(jnp.int32, (total, vocab), 1)
    hits = rows[:, 0:1] == ids
    e = jnp.sum(jnp.exp(capped), axis=1, keepdims=True)
    t = jnp.sum(jnp.where(hits, capped, 0.0), axis=1, keepdims=True)
    both = jnp.concatenate(
        [jnp.broadcast_to(e, (total, 128)), jnp.broadcast_to(t, (total, 128))], axis=0
    )
    sums[me] = jnp.transpose(both)[0:1, :]
    mark("sums")
    for d in range(1, n):
        pf, pm, ps = where_is(lax.rem(me + d, n))
        remote(sums.at[me], sums.at[me], sum_sem.at[0], sum_sem.at[1], pf, pm, ps).start()
    sum_all = sums.at[pl.ds(0, n - 1)]
    sum_in = remote(sum_all, sum_all, sum_sem.at[0], sum_sem.at[1], f, m, 1 - s)
    sum_in.wait_recv()
    mark("final")
    added = jnp.sum(sums[...], axis=0)
    pad = 2 * total
    spot = lax.broadcasted_iota(jnp.int32, (1, pad), 1)
    exp_sums = jnp.where(spot < total, added, 1.0)
    losses = weights * (jnp.log(exp_sums) - pltpu.roll(added, total, 1))
    mean = jnp.sum(losses, axis=1, keepdims=True) / jnp.maximum(
        jnp.sum(weights, axis=1, keepdims=True), 1.0
    )
    start = (s * nf + f) * tok
    mine_out = pltpu.roll(losses, lax.rem(pad - start, pad), 1)
    out[...] = jnp.where(spot < tok, mine_out, mean)[0, 0:out.shape[0]]

    mark("drain")
    for way in (0, 1):
        for j in range(1, nf):
            going = has_up if way == 0 else has_down

            @pl.when(jnp.logical_and(going, held(way, j - 1)))
            def _():
                remote(
                    gathered.at[0], gathered.at[0], hid_send.at[way, j - 1], hid_recv.at[0, 0], f, m, 1 - s
                ).wait_send()
    swap.wait_send()
    near_swap.wait_send()
    far_swap.wait_send()
    if nm > 1:
        peers(near_mid, near_mp).wait_send()
        peers(far_mid, far_mp).wait_send()
    res_in.wait_send()
    res_swap.wait_send()
    info_in.wait_send()
    mom_in.wait_send()
    mom_swap.wait_send()
    near_all = states.at[pl.ds(0, rest), 0, pl.ds(0, rest)]
    remote(near_all, near_all, near_send, near_recv.at[0], f, m, 1 - s).wait_send()
    far_all = states.at[pl.ds(0, rest), 0, 0]
    remote(far_all, far_all, far_send, far_recv.at[0], f, m, 1 - s).wait_send()
    near_all = states.at[:, 0, pl.ds(0, rest)]
    remote(near_all, near_all, near_fwd.at[nf], near_fwd.at[0], f, m, 1 - s).wait_send()
    far_all = states.at[:, 0, 0]
    remote(far_all, far_all, far_fwd.at[nf], far_fwd.at[0], f, m, 1 - s).wait_send()
    sum_in.wait_send()
    mark(None)


def finish(tok, row, losses, mean):
    losses[...] = row[0:tok]
    mean[...] = row[tok:tok + 1]


def on_device(
    nf, nm, hidden, residual, down_packed, down_scale, post_gain, final_gain, embed_packed, embed_scale,
    targets, loss_mask,
):
    tok, width_d = residual.shape
    rows, cols = down_packed.shape
    vocab, packed = embed_packed.shape
    half = rows // 2
    half_k = half * PLANES
    n = nf * nm * 2
    total = tok * 2 * nf
    rest = nf - 1
    groups = half_k // GROUP
    pieces = next(c for c in PIECES if groups % c == 0 and half_k // c % 256 == 0 or c == 1)
    piece = half_k // pieces
    width = 256 if piece % 256 == 0 else GROUP
    vm = pl.BlockSpec(memory_space=pltpu.VMEM)
    hbm = pl.BlockSpec(memory_space=pltpu.HBM)
    dma = pltpu.SemaphoreType.DMA
    bf16, f32, i32 = jnp.bfloat16, jnp.float32, jnp.int32
    row = pl.pallas_call(
        functools.partial(kernel, nf, nm),
        out_shape=jax.ShapeDtypeStruct((128,), f32),
        in_specs=[hbm] * 10,
        out_specs=vm,
        scratch_shapes=[
            pltpu.VMEM(hidden.shape, bf16),
            pltpu.VMEM(residual.shape, bf16),
            pltpu.VMEM((half, cols), i32),
            pltpu.VMEM(down_scale.shape, bf16),
            pltpu.VMEM((width_d,), f32),
            pltpu.VMEM((width_d,), f32),
            pltpu.VMEM((packed, vocab), i32),
            pltpu.VMEM((embed_scale.shape[1], vocab), bf16),
            pltpu.SMEM((tok,), i32),
            pltpu.SMEM((tok,), i32),
            pltpu.VMEM(down_scale.shape, f32),
            pltpu.VMEM((embed_scale.shape[1], vocab), f32),
            pltpu.VMEM((nf, 1, cols), f32),
            pltpu.VMEM((nf, 1, cols), f32),
            pltpu.VMEM((half_k, cols), bf16),
            pltpu.VMEM((width_d, vocab), bf16),
            pltpu.VMEM((width, width), bf16),
            pltpu.VMEM((2, pieces, tok, piece), bf16),
            pltpu.VMEM((nf, pieces, 2, tok, piece), bf16),
            pltpu.VMEM((2, rest * tok, cols), f32),
            pltpu.VMEM((rest * tok, cols), f32),
            pltpu.VMEM((rest * tok, cols), f32),
            pltpu.VMEM((nm, rest * tok, cols), f32),
            pltpu.VMEM((2, tok, cols), f32),
            pltpu.VMEM((tok, cols), f32),
            pltpu.VMEM((tok, cols), f32),
            pltpu.VMEM((nm, tok, cols), f32),
            pltpu.VMEM((nf, tok, cols), f32),
            pltpu.VMEM((2, nf, nf, tok, cols), bf16),
            pltpu.VMEM((nf, 2, nf, tok, cols), bf16),
            pltpu.VMEM((nf, nf * tok, 128), f32),
            pltpu.VMEM((2, nf * tok, 128), f32),
            pltpu.VMEM((tok, 128), i32),
            pltpu.VMEM((n, tok, 128), i32),
            pltpu.VMEM((n, 1, 2 * total), f32),
            dma((10,)),
            dma((2, max(nf - 1, 1))), dma((nf, pieces)),
            dma((2,)), dma((2,)), dma((2,)), dma((2,)), dma((2,)),
            dma((4,)), dma((2,)),
            dma, dma((nf,)), dma, dma((nf,)), dma((nf + 1,)), dma((nf + 1,)),
            dma((4,)), dma((2,)),
        ],
        compiler_params=pltpu.CompilerParams(
            collective_id=0, has_side_effects=True, vmem_limit_bytes=60 * 1024 * 1024
        ),
    )(
        hidden, residual, down_packed, down_scale, post_gain, final_gain,
        embed_packed.T, embed_scale.T, targets, loss_mask,
    )
    return pl.pallas_call(
        functools.partial(finish, tok),
        out_shape=(jax.ShapeDtypeStruct((tok,), f32), jax.ShapeDtypeStruct((1,), f32)),
        in_specs=[vm],
        out_specs=(vm, vm),
    )(row)


def solution(mesh):
    nf, nm = mesh.shape["fsdp"], mesh.shape["mp"]
    return jax.shard_map(
        functools.partial(on_device, nf, nm),
        mesh=mesh,
        in_specs=(
            P(("groups", "fsdp", "sub"), "mp"),
            P(("groups", "fsdp", "sub"), None),
            P("mp", "fsdp"),
            P("mp", "fsdp"),
            P(),
            P(),
            P(("fsdp", "mp", "sub"), None),
            P(("fsdp", "mp", "sub"), None),
            P(("groups", "fsdp", "sub")),
            P(("groups", "fsdp", "sub")),
        ),
        out_specs=(P(("groups", "fsdp", "sub")), P("groups")),
        check_vma=False,
    )
```

```python
import functools

import jax
import jax.numpy as jnp
from jax import lax
from jax.experimental import pallas as pl
from jax.experimental.pallas import tpu as pltpu
from jax.sharding import PartitionSpec as P

EPS = 1e-06
CAP = 30.0
MESH = pl.DeviceIdType.MESH
PLANES = 8
GROUP = 128
PIECES = (9, 8, 6, 4, 3, 2, 1)


def remote(src, dst, send, recv, f, m, s):
    return pltpu.make_async_remote_copy(
        src_ref=src,
        dst_ref=dst,
        send_sem=send,
        recv_sem=recv,
        device_id={"fsdp": f, "mp": m, "sub": s},
        device_id_type=MESH,
    )


def mark(name):
    pass


def kernel(
    nf, nm, hidden_hbm, residual_hbm, words_hbm, scale_hbm, post_hbm, final_hbm, embed_hbm, embed_scale_hbm,
    targets_hbm, mask_hbm,
    out,
    hidden, residual, words, scale, post_gain, final_gain, embed_words, embed_scale, targets, mask,
    scale_f, embed_f, post_z, final_z, weight, embed, perm, sorted_own, gathered,
    near_own, near_in, near_part, near_mid, far_own, far_in, far_part, far_mid,
    ffn, res, states, moments, moment, ratio, split, info, infos, sums,
    local_sem, hid_send, hid_recv, pair_sem, near_sem, far_sem, near_mp, far_mp, res_sem, res_recv, info_sem,
    near_send, near_recv, far_send, far_recv, near_fwd, far_fwd, mom_sem, sum_sem,
):
    f, m, s = lax.axis_index("fsdp"), lax.axis_index("mp"), lax.axis_index("sub")
    n = nf * nm * 2
    me = (f * nm + m) * 2 + s
    tok = hidden.shape[0]
    half_rows, cols = words.shape
    half_k = half_rows * PLANES
    total = tok * 2 * nf
    width_d = nf * cols
    pieces, piece = gathered.shape[1], gathered.shape[4]
    groups = half_k // GROUP
    per = GROUP // PLANES
    rest = nf - 1
    low = f < nf - nf // 2
    far = jnp.where(low, nf - 1, 0)
    first = jnp.where(low, 0, 1)
    up, down = lax.rem(f + 1, nf), lax.rem(f + nf - 1, nf)
    has_up, has_down = f < nf - 1, f > 0
    inner = jnp.logical_and(has_up, has_down)

    def where_is(q):
        return q // (2 * nm), (q // 2) % nm, q % 2

    barrier = pltpu.get_barrier_semaphore()

    def greet(pf, pm, ps):
        pl.semaphore_signal(
            barrier, inc=1, device_id={"fsdp": pf, "mp": pm, "sub": ps}, device_id_type=MESH
        )

    @pl.when(has_up)
    def _():
        greet(up, m, 0)
        greet(up, m, 1)

    @pl.when(has_down)
    def _():
        greet(down, m, 0)
        greet(down, m, 1)

    greet(f, m, 1 - s)
    for d in range(1, nm):
        greet(f, lax.rem(m + d, nm), s)

    def load(i, src, dst):
        copy = pltpu.make_async_copy(src, dst, local_sem.at[i])
        copy.start()
        return copy

    load_hidden = load(0, hidden_hbm, hidden)
    load_residual = load(5, residual_hbm, residual)
    load_words = load(
        1, words_hbm.at[pl.ds(pl.multiple_of(s * half_rows, 8), half_rows)], words
    )
    load_scale = load(2, scale_hbm, scale)
    loads = [
        load(3, embed_hbm, embed_words), load(4, embed_scale_hbm, embed_scale),
        load(6, post_hbm, post_gain), load(7, final_hbm, final_gain),
        load(8, targets_hbm, targets), load(9, mask_hbm, mask),
    ]

    width = perm.shape[0]
    row = lax.broadcasted_iota(jnp.int32, (width, width), 0)
    col = lax.broadcasted_iota(jnp.int32, (width, width), 1)
    inside = jnp.bitwise_and(col, GROUP - 1)
    source = (col - inside) + jnp.bitwise_and(inside, per - 1) * PLANES + jnp.right_shift(inside, 4)
    perm[...] = jnp.where(row == source, 1.0, 0.0).astype(jnp.bfloat16)

    mark("hidden_wait")
    load_hidden.wait()
    mark("permute")
    own = hidden[...].astype(jnp.float32)
    spans = 2 * half_k // width
    stacked = jnp.concatenate(
        [own[:, c * width:(c + 1) * width] for c in range(spans)], axis=0
    ).astype(jnp.bfloat16)
    ordered = jnp.dot(stacked, perm[...], preferred_element_type=jnp.float32)
    for c in range(spans):
        h, at = c * width // half_k, c * width % half_k
        sorted_own[h, at // piece, :, at % piece:at % piece + width] = ordered[
            c * tok:(c + 1) * tok
        ].astype(jnp.bfloat16)

    mark("barrier")
    count = 1 + (nm - 1) + 2 * has_up.astype(jnp.int32) + 2 * has_down.astype(jnp.int32)
    pl.semaphore_wait(barrier, count)
    mark("send1")

    def first_hop(way, i):
        target = up if way == 0 else down
        for h in (0, 1):
            remote(
                sorted_own.at[h, i], gathered.at[f, i, s], hid_send.at[way, 0], hid_recv.at[f, i],
                target, m, h,
            ).start()

    def block_at(way, j):
        return lax.rem(f - j + nf, nf) if way == 0 else lax.rem(f + j, nf)

    def held(way, j):
        return f >= j if way == 0 else f + j <= nf - 1

    def arrive(b, i):
        remote(
            gathered.at[b, i], gathered.at[b, i], hid_send.at[0, 0], hid_recv.at[b, i], f, m, 1 - s
        ).wait_recv()

    def pass_on(j, i):
        for way in (0, 1):
            b = block_at(way, j)
            target = up if way == 0 else down

            @pl.when(jnp.logical_and(inner, held(way, j)))
            def _():
                arrive(b, i)
                remote(
                    gathered.at[b, i], gathered.at[b, i], hid_send.at[way, j], hid_recv.at[b, i],
                    target, m, s,
                ).start()

    for i in range(pieces):
        @pl.when(has_up)
        def _():
            first_hop(0, i)

        @pl.when(has_down)
        def _():
            first_hop(1, i)

    swap = remote(
        sorted_own.at[1 - s], gathered.at[f, :, s], pair_sem.at[0], pair_sem.at[1], f, m, 1 - s
    )
    swap.start()
    gathered[f, :, s] = sorted_own[s]
    load_residual.wait()
    own_res = residual[...].astype(jnp.float32)
    for z in range(nf):
        res[s, f, z] = own_res[:, z * cols:(z + 1) * cols].astype(jnp.bfloat16)

    def late(way):
        return jnp.logical_and(inner, (f == nf - 2) if way == 0 else (f == 1))

    def res_arrive(b):
        ref = res.at[s, b]
        remote(ref, ref, res_sem.at[0], res_recv.at[b], f, m, 1 - s).wait_recv()

    def res_send(way, j, when):
        b = block_at(way, j)
        going = has_up if way == 0 else has_down

        @pl.when(jnp.logical_and(jnp.logical_and(going, held(way, j)), when))
        def _():
            if j > 0:
                res_arrive(b)
            remote(
                res.at[s, b], res.at[s, b], res_sem.at[2 + way * nf + j], res_recv.at[b],
                up if way == 0 else down, m, s,
            ).start()

    for way in (0, 1):
        res_send(way, 0, jnp.logical_not(inner))

    mark("deq")
    load_scale.wait()
    scale_f[...] = scale[...].astype(jnp.float32)
    load_words.wait()

    def dequant(g, carry):
        w = words[pl.ds(pl.multiple_of(g * per, per), per), :]
        sc = scale_f[pl.ds(s * groups + g, 1), :]
        for k in range(PLANES):
            code = jnp.right_shift(jnp.left_shift(w, 28 - 4 * k), 28) if k < 7 else jnp.right_shift(w, 28)
            weight[pl.ds(pl.multiple_of(g * GROUP + k * per, per), per), :] = (
                code.astype(jnp.float32) * sc
            ).astype(jnp.bfloat16)
        return carry

    each = groups // pieces
    lag = min(3, pieces)
    for i in range(pieces):
        lax.fori_loop(i * each, (i + 1) * each, dequant, 0)
        if i >= lag and nf > 2:
            pass_on(1, i - lag)

    mark("deqE")
    for copy in loads:
        copy.wait()
    embed_f[...] = embed_scale[...].astype(jnp.float32)
    packed, vocab = embed_words.shape
    span = packed * PLANES // embed_f.shape[0]
    step = 32
    blocks = packed // step

    def dequant_embed(i, carry):
        w = embed_words[pl.ds(pl.multiple_of(i * step, step), step), :]
        for k in range(PLANES):
            code = jnp.right_shift(jnp.left_shift(w, 28 - 4 * k), 28) if k < 7 else jnp.right_shift(w, 28)
            sc = embed_f[pl.ds((k * packed + i * step) // span, 1), :]
            embed[pl.ds(pl.multiple_of(k * packed + i * step, step), step), :] = (
                code.astype(jnp.float32) * sc
            ).astype(jnp.bfloat16)
        return carry

    def dequant_some(part, parts):
        lax.fori_loop(part * blocks // parts, (part + 1) * blocks // parts, dequant_embed, 0)

    for part in range(lag):
        dequant_some(part, lag)
        if nf > 2:
            pass_on(1, pieces - lag + part)
    for j in range(2, nf - 2):
        for i in range(pieces):
            pass_on(j, i)

    mark("prep")
    post_row, final_row = post_gain[...].reshape(1, width_d), final_gain[...].reshape(1, width_d)
    for z in range(nf):
        post_z[z] = post_row[:, z * cols:(z + 1) * cols]
        final_z[z] = final_row[:, z * cols:(z + 1) * cols]
    side = lax.broadcasted_iota(jnp.int32, (1, 128), 1)
    entry = jnp.zeros((1, 128), jnp.int32)
    for i in range(tok):
        entry = jnp.where(side == i, targets[i], jnp.where(side == 64 + i, mask[i], entry))
    info[...] = entry
    infos[s * nf + f] = entry

    for j in range(rest):
        for way in (0, 1):
            res_send(way, j, jnp.logical_and(inner, jnp.logical_not(late(way))))

    mark("near_mm")
    swap.wait_recv()
    edge = jnp.logical_not(inner)
    near_acc = jnp.zeros((rest * 2 * tok, cols), jnp.float32)
    for i in range(pieces):
        if nf > 3:
            pass_on(nf - 2, i)
        for b in range(nf):
            @pl.when(jnp.logical_and(edge, jnp.logical_and(f != b, far != b)))
            def _():
                arrive(b, i)

        lhs = gathered[pl.ds(first, rest), i].astype(jnp.float32).reshape(
            rest * 2 * tok, piece
        ).astype(jnp.bfloat16)
        near_acc = near_acc + jnp.dot(
            lhs, weight[i * piece:(i + 1) * piece], preferred_element_type=jnp.float32
        )
    for b in range(rest):
        for h in (0, 1):
            at = (2 * b + h) * tok
            near_own[h, b * tok:(b + 1) * tok] = near_acc[at:at + tok]
    near_swap = remote(
        near_own.at[1 - s], near_in, near_sem.at[0], near_sem.at[1], f, m, 1 - s
    )
    near_swap.start()
    for way in (0, 1):
        res_send(way, 0, late(way))

    def to_peers(part, mid, sems):
        for d in range(1, nm):
            remote(
                part, mid.at[m], sems.at[0], sems.at[1], f, lax.rem(m + d, nm), s
            ).start()

    def peers(mid, sems):
        ref = mid.at[pl.ds(0, nm - 1)]
        return remote(ref, ref, sems.at[0], sems.at[1], f, m, 1 - s)

    def gather_peers(part, mid, sems):
        if nm > 1:
            peers(mid, sems).wait_recv()
        full = part[...]
        for d in range(1, nm):
            full = full + mid[lax.rem(m + d, nm)]
        return full

    def nearer(d):
        return jnp.where(low, lax.rem(f + d, nf), lax.rem(f + nf - d, nf))

    def early_sends():
        spot = infos.at[s * nf + f]
        for d in range(1, nf):
            for h in (0, 1):
                remote(info, spot, info_sem.at[0], info_sem.at[1], lax.rem(f + d, nf), m, h).start()
        remote(info, spot, info_sem.at[0], info_sem.at[1], f, m, 1 - s).start()

    mark("far_mm")
    far_acc = jnp.zeros((2 * tok, cols), jnp.float32)
    reduce_at, send_at = min(2, pieces - 1), min(6, pieces - 1)
    for i in range(pieces):
        @pl.when(edge)
        def _():
            arrive(far, i)

        lhs = gathered[far, i].astype(jnp.float32).reshape(2 * tok, piece).astype(jnp.bfloat16)
        far_acc = far_acc + jnp.dot(
            lhs, weight[i * piece:(i + 1) * piece], preferred_element_type=jnp.float32
        )
        if i == reduce_at:
            near_swap.wait_recv()
            near_part[...] = near_own[s] + near_in[...]
            to_peers(near_part, near_mid, near_mp)
        if i == send_at:
            early_sends()
        for j in range(1, rest):
            if i == min(send_at - 1 + 2 * j, pieces - 1):
                for way in (0, 1):
                    res_send(way, j, late(way))
    for h in (0, 1):
        far_own[h] = far_acc[h * tok:(h + 1) * tok]
    mark("far_swap")
    far_swap = remote(far_own.at[1 - s], far_in, far_sem.at[0], far_sem.at[1], f, m, 1 - s)
    far_swap.start()

    near_ffn = gather_peers(near_part, near_mid, near_mp)
    ffn[pl.ds(first, rest)] = near_ffn.reshape(rest, tok, cols)
    gains = post_z[f] * final_z[f]
    near_at = pl.ds(first, rest)
    states[f, s, near_at] = (near_ffn * gains).reshape(rest, tok, cols).astype(jnp.bfloat16)

    def near_to(z, pf, ps, send, recv):
        return remote(
            states.at[z, s, near_at], states.at[z, s, near_at], send, recv, pf, m, ps
        )

    def near_span(z):
        return pl.ds(jnp.where(z < nf - nf // 2, 0, 1), rest)

    def far_spot(z):
        return jnp.where(z < nf - nf // 2, nf - 1, 0)

    for d in range(rest, 0, -1):
        near_to(f, nearer(d), s, near_send, near_recv.at[f]).start()
    near_to(f, f, 1 - s, near_fwd.at[nf], near_fwd.at[f]).start()

    mark("far_in")
    far_swap.wait_recv()
    far_part[...] = far_own[s] + far_in[...]
    to_peers(far_part, far_mid, far_mp)
    mark("far_mp")
    far_ffn = gather_peers(far_part, far_mid, far_mp)
    ffn[far] = far_ffn
    states[f, s, far] = (far_ffn * gains).astype(jnp.bfloat16)

    def far_to(z, pf, ps, send, recv):
        spot = far_spot(z)
        return remote(states.at[z, s, spot], states.at[z, s, spot], send, recv, pf, m, ps)

    for d in range(rest, 0, -1):
        far_to(f, nearer(d), s, far_send, far_recv.at[f]).start()
    far_to(f, f, 1 - s, far_fwd.at[nf], far_fwd.at[f]).start()

    mark("moments")
    mine = nf * tok
    y = ffn[...].reshape(mine, cols)
    g = y * post_z[f]
    lane = lax.broadcasted_iota(jnp.int32, (mine, 128), 1)

    def row_sum(v):
        return jnp.sum(v, axis=1, keepdims=True)

    def tall(v):
        extra = 128 - v.shape[0]
        return v if extra == 0 else jnp.concatenate([v, jnp.zeros((extra, 128), jnp.float32)], axis=0)

    moments[f] = jnp.transpose(tall(jnp.where(lane < 1, row_sum(y * y), row_sum(g * g))))[0:8]
    for d in range(rest, 0, -1):
        remote(moments.at[f], moments.at[f], mom_sem.at[0], mom_sem.at[1], nearer(d), m, s).start()

    def same(z, span, sems, recv):
        ref = states.at[z, s, span]
        return remote(ref, ref, sems, recv, f, m, 1 - s)

    def other(z, span, sems, recv):
        ref = states.at[z, 1 - s, span]
        return remote(ref, ref, sems, recv, f, m, 1 - s)

    def hand_near(d):
        z = nearer(d)
        same(z, near_span(z), near_send, near_recv.at[z]).wait_recv()
        same(z, near_span(z), near_fwd.at[nf], near_fwd.at[z]).start()

    def hand_far(d):
        z = nearer(d)
        same(z, far_spot(z), far_send, far_recv.at[z]).wait_recv()
        same(z, far_spot(z), far_fwd.at[nf], far_fwd.at[z]).start()

    def product(d):
        z = nearer(d)
        other(z, near_span(z), near_fwd.at[nf], near_fwd.at[z]).wait_recv()
        other(z, far_spot(z), far_fwd.at[nf], far_fwd.at[z]).wait_recv()
        wide = states[z].astype(jnp.float32).reshape(total, cols)
        cross = row_sum(wide * ratio[z])
        return cross, jnp.dot(
            jnp.concatenate([split[z], wide.astype(jnp.bfloat16)], axis=0), embed[pl.ds(pl.multiple_of(z * cols, 32), cols), :],
            preferred_element_type=jnp.float32,
        )

    mark("info")
    info_all = infos.at[pl.ds(0, 2 * nf - 1)]
    info_in = remote(info_all, info_all, info_sem.at[0], info_sem.at[1], f, m, 1 - s)
    info_in.wait_recv()
    turned = jnp.transpose(tall(infos[...].astype(jnp.float32).reshape(2 * nf, 128)))
    wanted = jnp.concatenate([turned[0:tok, e:e + 1] for e in range(2 * nf)], axis=0).astype(jnp.int32)
    counted = jnp.concatenate([turned[64:64 + tok, e:e + 1] for e in range(2 * nf)], axis=0)
    weights = jnp.transpose(
        jnp.concatenate(
            [jnp.broadcast_to(counted, (total, 128)), jnp.zeros((total, 128), jnp.float32)], axis=0
        )
    )[0:1, :]

    mark("res_wait")

    for b in range(nf):
        @pl.when(jnp.logical_and(edge, f != b))
        def _():
            res_arrive(b)

    res_swap = remote(res.at[s], res.at[s], res_sem.at[0], res_sem.at[1], f, m, 1 - s)
    res_swap.start()
    mark("near_fwd1")
    for d in range(1, rest):
        hand_near(d)
    mark("near_fwd2")
    hand_near(rest)
    hand_far(1)
    mark("logits0")
    res_other = res.at[1 - s]
    remote(res_other, res_other, res_sem.at[0], res_sem.at[1], f, m, 1 - s).wait_recv()
    power = jnp.zeros((total, 1), jnp.float32)
    for z in range(nf):
        rz = res[:, :, z].astype(jnp.float32).reshape(total, cols)
        power = power + row_sum(rz * rz)
        ratio[z] = rz / final_z[z]
        rf = rz * final_z[z]
        high = rf.astype(jnp.bfloat16)
        split[z, 0:total] = high
        split[z, total:2 * total] = (rf - high.astype(jnp.float32)).astype(jnp.bfloat16)

    mark("far_fwd")
    for d in range(2, nf):
        hand_far(d)
    mark("moments_in")
    mom_all = moments.at[pl.ds(0, rest)]
    mom_in = remote(mom_all, mom_all, mom_sem.at[0], mom_sem.at[1], f, m, 1 - s)
    mom_in.wait_recv()
    moment[s] = jnp.sum(moments[...], axis=0)
    mom_swap = remote(moment.at[s], moment.at[s], mom_sem.at[2], mom_sem.at[3], f, m, 1 - s)
    mom_swap.start()

    mark("logits1")
    cross, main = product(0)
    for d in range(1, rest):
        more, term = product(d)
        cross, main = cross + more, main + term
    mark("last")
    moment_other = moment.at[1 - s]
    remote(
        moment_other, moment_other, mom_sem.at[2], mom_sem.at[3], f, m, 1 - s
    ).wait_recv()
    turned = jnp.transpose(tall(moment[...].reshape(16, 128)))

    def column(q):
        return jnp.concatenate([turned[0:mine, q:q + 1], turned[0:mine, q + 8:q + 9]], axis=0)

    inv = lax.rsqrt(column(0) / width_d + EPS)
    square = power + inv * inv * column(1)
    mark("logits2")
    if rest > 0:
        more, term = product(rest)
        cross, main = cross + more, main + term
    inv2 = lax.rsqrt((square + 2.0 * inv * cross) / width_d + EPS)
    logits = (main[0:total] + main[total:2 * total] + main[2 * total:] * inv) * inv2
    capped = CAP * jnp.tanh(logits / CAP)
    ids = me * vocab + lax.broadcasted_iota(jnp.int32, (total, vocab), 1)
    hits = wanted == ids
    e = jnp.sum(jnp.exp(capped), axis=1, keepdims=True)
    t = jnp.sum(jnp.where(hits, capped, 0.0), axis=1, keepdims=True)
    both = jnp.concatenate(
        [jnp.broadcast_to(e, (total, 128)), jnp.broadcast_to(t, (total, 128))], axis=0
    )
    sums[me] = jnp.transpose(both)[0:1, :]
    mark("sums")
    for d in range(1, n):
        pf, pm, ps = where_is(lax.rem(me + d, n))
        remote(sums.at[me], sums.at[me], sum_sem.at[0], sum_sem.at[1], pf, pm, ps).start()
    sum_all = sums.at[pl.ds(0, n - 1)]
    sum_in = remote(sum_all, sum_all, sum_sem.at[0], sum_sem.at[1], f, m, 1 - s)
    sum_in.wait_recv()
    mark("final")
    added = jnp.sum(sums[...], axis=0)
    pad = 2 * total
    spot = lax.broadcasted_iota(jnp.int32, (1, pad), 1)
    exp_sums = jnp.where(spot < total, added, 1.0)
    losses = weights * (jnp.log(exp_sums) - pltpu.roll(added, total, 1))
    mean = jnp.sum(losses, axis=1, keepdims=True) / jnp.maximum(
        jnp.sum(weights, axis=1, keepdims=True), 1.0
    )
    start = (s * nf + f) * tok
    mine_out = pltpu.roll(losses, lax.rem(pad - start, pad), 1)
    out[...] = jnp.where(spot < tok, mine_out, mean)[0, 0:out.shape[0]]

    mark("drain")
    for way in (0, 1):
        for j in range(1, nf):
            going = has_up if way == 0 else has_down

            @pl.when(jnp.logical_and(going, held(way, j - 1)))
            def _():
                remote(
                    gathered.at[0], gathered.at[0], hid_send.at[way, j - 1], hid_recv.at[0, 0], f, m, 1 - s
                ).wait_send()
    swap.wait_send()
    near_swap.wait_send()
    far_swap.wait_send()
    if nm > 1:
        peers(near_mid, near_mp).wait_send()
        peers(far_mid, far_mp).wait_send()
    for way in (0, 1):
        for j in range(rest):
            going = has_up if way == 0 else has_down

            @pl.when(jnp.logical_and(going, held(way, j)))
            def _():
                remote(
                    res.at[s, 0], res.at[s, 0], res_sem.at[2 + way * nf + j], res_recv.at[0], f, m, 1 - s
                ).wait_send()

    res_swap.wait_send()
    info_in.wait_send()
    mom_in.wait_send()
    mom_swap.wait_send()
    near_all = states.at[pl.ds(0, rest), 0, pl.ds(0, rest)]
    remote(near_all, near_all, near_send, near_recv.at[0], f, m, 1 - s).wait_send()
    far_all = states.at[pl.ds(0, rest), 0, 0]
    remote(far_all, far_all, far_send, far_recv.at[0], f, m, 1 - s).wait_send()
    near_all = states.at[:, 0, pl.ds(0, rest)]
    remote(near_all, near_all, near_fwd.at[nf], near_fwd.at[0], f, m, 1 - s).wait_send()
    far_all = states.at[:, 0, 0]
    remote(far_all, far_all, far_fwd.at[nf], far_fwd.at[0], f, m, 1 - s).wait_send()
    sum_in.wait_send()
    mark(None)


def finish(tok, row, losses, mean):
    losses[...] = row[0:tok]
    mean[...] = row[tok:tok + 1]


def on_device(
    nf, nm, hidden, residual, down_packed, down_scale, post_gain, final_gain, embed_packed, embed_scale,
    targets, loss_mask,
):
    tok, width_d = residual.shape
    rows, cols = down_packed.shape
    vocab, packed = embed_packed.shape
    half = rows // 2
    half_k = half * PLANES
    n = nf * nm * 2
    total = tok * 2 * nf
    rest = nf - 1
    groups = half_k // GROUP
    pieces = next(c for c in PIECES if groups % c == 0 and half_k // c % 256 == 0 or c == 1)
    piece = half_k // pieces
    width = 256 if piece % 256 == 0 else GROUP
    vm = pl.BlockSpec(memory_space=pltpu.VMEM)
    hbm = pl.BlockSpec(memory_space=pltpu.HBM)
    dma = pltpu.SemaphoreType.DMA
    bf16, f32, i32 = jnp.bfloat16, jnp.float32, jnp.int32
    row = pl.pallas_call(
        functools.partial(kernel, nf, nm),
        out_shape=jax.ShapeDtypeStruct((128,), f32),
        in_specs=[hbm] * 10,
        out_specs=vm,
        scratch_shapes=[
            pltpu.VMEM(hidden.shape, bf16),
            pltpu.VMEM(residual.shape, bf16),
            pltpu.VMEM((half, cols), i32),
            pltpu.VMEM(down_scale.shape, bf16),
            pltpu.VMEM((width_d,), f32),
            pltpu.VMEM((width_d,), f32),
            pltpu.VMEM((packed, vocab), i32),
            pltpu.VMEM((embed_scale.shape[1], vocab), bf16),
            pltpu.SMEM((tok,), i32),
            pltpu.SMEM((tok,), i32),
            pltpu.VMEM(down_scale.shape, f32),
            pltpu.VMEM((embed_scale.shape[1], vocab), f32),
            pltpu.VMEM((nf, 1, cols), f32),
            pltpu.VMEM((nf, 1, cols), f32),
            pltpu.VMEM((half_k, cols), bf16),
            pltpu.VMEM((width_d, vocab), bf16),
            pltpu.VMEM((width, width), bf16),
            pltpu.VMEM((2, pieces, tok, piece), bf16),
            pltpu.VMEM((nf, pieces, 2, tok, piece), bf16),
            pltpu.VMEM((2, rest * tok, cols), f32),
            pltpu.VMEM((rest * tok, cols), f32),
            pltpu.VMEM((rest * tok, cols), f32),
            pltpu.VMEM((nm, rest * tok, cols), f32),
            pltpu.VMEM((2, tok, cols), f32),
            pltpu.VMEM((tok, cols), f32),
            pltpu.VMEM((tok, cols), f32),
            pltpu.VMEM((nm, tok, cols), f32),
            pltpu.VMEM((nf, tok, cols), f32),
            pltpu.VMEM((2, nf, nf, tok, cols), bf16),
            pltpu.VMEM((nf, 2, nf, tok, cols), bf16),
            pltpu.VMEM((nf, 8, 128), f32),
            pltpu.VMEM((2, 8, 128), f32),
            pltpu.VMEM((nf, total, cols), f32),
            pltpu.VMEM((nf, 2 * total, cols), bf16),
            pltpu.VMEM((1, 128), i32),
            pltpu.VMEM((2 * nf, 1, 128), i32),
            pltpu.VMEM((n, 1, 2 * total), f32),
            dma((10,)),
            dma((2, max(nf - 1, 1))), dma((nf, pieces)),
            dma((2,)), dma((2,)), dma((2,)), dma((2,)), dma((2,)),
            dma((2 + 2 * nf,)), dma((nf,)), dma((2,)),
            dma, dma((nf,)), dma, dma((nf,)), dma((nf + 1,)), dma((nf + 1,)),
            dma((4,)), dma((2,)),
        ],
        compiler_params=pltpu.CompilerParams(
            collective_id=0, has_side_effects=True, vmem_limit_bytes=60 * 1024 * 1024
        ),
    )(
        hidden, residual, down_packed, down_scale, post_gain, final_gain,
        embed_packed.T, embed_scale.T, targets, loss_mask,
    )
    return pl.pallas_call(
        functools.partial(finish, tok),
        out_shape=(jax.ShapeDtypeStruct((tok,), f32), jax.ShapeDtypeStruct((1,), f32)),
        in_specs=[vm],
        out_specs=(vm, vm),
    )(row)


def solution(mesh):
    nf, nm = mesh.shape["fsdp"], mesh.shape["mp"]
    return jax.shard_map(
        functools.partial(on_device, nf, nm),
        mesh=mesh,
        in_specs=(
            P(("groups", "fsdp", "sub"), "mp"),
            P(("groups", "fsdp", "sub"), None),
            P("mp", "fsdp"),
            P("mp", "fsdp"),
            P(),
            P(),
            P(("fsdp", "mp", "sub"), None),
            P(("fsdp", "mp", "sub"), None),
            P(("groups", "fsdp", "sub")),
            P(("groups", "fsdp", "sub")),
        ),
        out_specs=(P(("groups", "fsdp", "sub")), P("groups")),
        check_vma=False,
    )
```

```python
import functools

import jax
import jax.numpy as jnp
from jax import lax
from jax.experimental import pallas as pl
from jax.experimental.pallas import tpu as pltpu
from jax.sharding import PartitionSpec as P

EPS = 1e-06
CAP = 30.0
MESH = pl.DeviceIdType.MESH
PLANES = 8
GROUP = 128
PIECES = (9, 8, 6, 4, 3, 2, 1)


def remote(src, dst, send, recv, f, m, s):
    return pltpu.make_async_remote_copy(
        src_ref=src,
        dst_ref=dst,
        send_sem=send,
        recv_sem=recv,
        device_id={"fsdp": f, "mp": m, "sub": s},
        device_id_type=MESH,
    )


def mark(name):
    pass


def kernel(
    nf, nm, hidden_hbm, residual_hbm, words_hbm, scale_hbm, post_hbm, final_hbm, embed_hbm, embed_scale_hbm,
    targets_hbm, mask_hbm,
    out,
    hidden, residual, words, scale, post_gain, final_gain, embed_words, embed_scale, targets, mask,
    scale_f, embed_f, post_z, final_z, weight, embed, perm, sorted_own, gathered,
    near_own, near_in, near_part, near_mid, far_own, far_mid,
    ffn, res, states, moments, ratio, base_sum, power_sum, info, infos, sums,
    local_sem, hid_send, hid_recv, pair_sem, near_sem, near_mp, far_mp, res_sem, res_recv, info_sem,
    near_send, near_recv, far_send, far_recv, near_fwd, mom_sem, sum_sem,
):
    f, m, s = lax.axis_index("fsdp"), lax.axis_index("mp"), lax.axis_index("sub")
    n = nf * nm * 2
    me = (f * nm + m) * 2 + s
    tok = hidden.shape[0]
    half_rows, cols = words.shape
    half_k = half_rows * PLANES
    total = tok * 2 * nf
    width_d = nf * cols
    pieces, piece = gathered.shape[1], gathered.shape[4]
    groups = half_k // GROUP
    per = GROUP // PLANES
    rest = nf - 1
    low = f < nf - nf // 2
    far = jnp.where(low, nf - 1, 0)
    first = jnp.where(low, 0, 1)
    up, down = lax.rem(f + 1, nf), lax.rem(f + nf - 1, nf)
    has_up, has_down = f < nf - 1, f > 0
    inner = jnp.logical_and(has_up, has_down)

    def where_is(q):
        return q // (2 * nm), (q // 2) % nm, q % 2

    barrier = pltpu.get_barrier_semaphore()

    def greet(pf, pm, ps):
        pl.semaphore_signal(
            barrier, inc=1, device_id={"fsdp": pf, "mp": pm, "sub": ps}, device_id_type=MESH
        )

    @pl.when(has_up)
    def _():
        greet(up, m, 0)
        greet(up, m, 1)

    @pl.when(has_down)
    def _():
        greet(down, m, 0)
        greet(down, m, 1)

    greet(f, m, 1 - s)
    for d in range(1, nm):
        greet(f, lax.rem(m + d, nm), s)

    def load(i, src, dst):
        copy = pltpu.make_async_copy(src, dst, local_sem.at[i])
        copy.start()
        return copy

    load_hidden = load(0, hidden_hbm, hidden)
    load_residual = load(5, residual_hbm, residual)
    load_words = load(
        1, words_hbm.at[pl.ds(pl.multiple_of(s * half_rows, 8), half_rows)], words
    )
    load_scale = load(2, scale_hbm, scale)
    loads = [
        load(3, embed_hbm, embed_words), load(4, embed_scale_hbm, embed_scale),
        load(6, post_hbm, post_gain), load(7, final_hbm, final_gain),
        load(8, targets_hbm, targets), load(9, mask_hbm, mask),
    ]

    width = perm.shape[0]
    row = lax.broadcasted_iota(jnp.int32, (width, width), 0)
    col = lax.broadcasted_iota(jnp.int32, (width, width), 1)
    inside = jnp.bitwise_and(col, GROUP - 1)
    source = (col - inside) + jnp.bitwise_and(inside, per - 1) * PLANES + jnp.right_shift(inside, 4)
    perm[...] = jnp.where(row == source, 1.0, 0.0).astype(jnp.bfloat16)

    mark("hidden_wait")
    load_hidden.wait()
    mark("permute")
    own = hidden[...].astype(jnp.float32)
    spans = 2 * half_k // width
    stacked = jnp.concatenate(
        [own[:, c * width:(c + 1) * width] for c in range(spans)], axis=0
    ).astype(jnp.bfloat16)
    ordered = jnp.dot(stacked, perm[...], preferred_element_type=jnp.float32)
    for c in range(spans):
        h, at = c * width // half_k, c * width % half_k
        sorted_own[h, at // piece, :, at % piece:at % piece + width] = ordered[
            c * tok:(c + 1) * tok
        ].astype(jnp.bfloat16)

    mark("barrier")
    count = 1 + (nm - 1) + 2 * has_up.astype(jnp.int32) + 2 * has_down.astype(jnp.int32)
    pl.semaphore_wait(barrier, count)
    mark("send1")

    def first_hop(way, i):
        target = up if way == 0 else down
        for h in (0, 1):
            remote(
                sorted_own.at[h, i], gathered.at[f, i, s], hid_send.at[way, 0], hid_recv.at[f, i],
                target, m, h,
            ).start()

    def block_at(way, j):
        return lax.rem(f - j + nf, nf) if way == 0 else lax.rem(f + j, nf)

    def held(way, j):
        return f >= j if way == 0 else f + j <= nf - 1

    def arrive(b, i):
        remote(
            gathered.at[b, i], gathered.at[b, i], hid_send.at[0, 0], hid_recv.at[b, i], f, m, 1 - s
        ).wait_recv()

    def pass_on(j, i):
        for way in (0, 1):
            b = block_at(way, j)
            target = up if way == 0 else down

            @pl.when(jnp.logical_and(inner, held(way, j)))
            def _():
                arrive(b, i)
                remote(
                    gathered.at[b, i], gathered.at[b, i], hid_send.at[way, j], hid_recv.at[b, i],
                    target, m, s,
                ).start()

    for i in range(pieces):
        @pl.when(has_up)
        def _():
            first_hop(0, i)

        @pl.when(has_down)
        def _():
            first_hop(1, i)

    swap = remote(
        sorted_own.at[1 - s], gathered.at[f, :, s], pair_sem.at[0], pair_sem.at[1], f, m, 1 - s
    )
    swap.start()
    gathered[f, :, s] = sorted_own[s]
    load_residual.wait()
    own_res = residual[...].astype(jnp.float32)
    for z in range(nf):
        res[s, f, z] = own_res[:, z * cols:(z + 1) * cols].astype(jnp.bfloat16)

    halved = nf > 2 and nf % nm == 0
    span_z = nf // nm if halved else nf
    whole_z = pl.ds(0, nf)
    part_z = pl.ds(m * span_z, span_z) if halved else whole_z

    def share(d):
        return part_z if d < rest else whole_z

    def late(way):
        return jnp.logical_and(inner, (f == nf - 2) if way == 0 else (f == 1))

    def res_arrive(b, zs):
        ref = res.at[s, b, zs]
        remote(ref, ref, res_sem.at[0], res_recv.at[b], f, m, 1 - s).wait_recv()

    def res_send(way, j, when, zs=pl.ds(0, nf)):
        b = block_at(way, j)
        going = has_up if way == 0 else has_down

        @pl.when(jnp.logical_and(jnp.logical_and(going, held(way, j)), when))
        def _():
            if j > 0:
                res_arrive(b, pl.ds(0, nf))
            ref = res.at[s, b, zs]
            remote(
                ref, ref, res_sem.at[4 + way * nf + j], res_recv.at[b], up if way == 0 else down, m, s
            ).start()

    def res_pair(b, zs):
        ref = res.at[s, b, zs]
        remote(ref, ref, res_sem.at[0], res_sem.at[1], f, m, 1 - s).start()

    for way in (0, 1):
        res_send(way, 0, jnp.logical_not(inner))
    res_pair(f, pl.ds(0, nf))

    mark("deq")
    load_scale.wait()
    scale_f[...] = scale[...].astype(jnp.float32)
    load_words.wait()

    def dequant(g, carry):
        w = words[pl.ds(pl.multiple_of(g * per, per), per), :]
        sc = scale_f[pl.ds(s * groups + g, 1), :]
        for k in range(PLANES):
            code = jnp.right_shift(jnp.left_shift(w, 28 - 4 * k), 28) if k < 7 else jnp.right_shift(w, 28)
            weight[pl.ds(pl.multiple_of(g * GROUP + k * per, per), per), :] = (
                code.astype(jnp.float32) * sc
            ).astype(jnp.bfloat16)
        return carry

    each = groups // pieces
    lag = min(3, pieces)
    for i in range(pieces):
        lax.fori_loop(i * each, (i + 1) * each, dequant, 0)
        if i >= lag and nf > 2:
            pass_on(1, i - lag)

    mark("deqE")
    for copy in loads:
        copy.wait()
    embed_f[...] = embed_scale[...].astype(jnp.float32)
    packed, vocab = embed_words.shape
    span = packed * PLANES // embed_f.shape[0]
    step = 32
    blocks = packed // step

    def dequant_embed(i, carry):
        w = embed_words[pl.ds(pl.multiple_of(i * step, step), step), :]
        for k in range(PLANES):
            code = jnp.right_shift(jnp.left_shift(w, 28 - 4 * k), 28) if k < 7 else jnp.right_shift(w, 28)
            sc = embed_f[pl.ds((k * packed + i * step) // span, 1), :]
            embed[pl.ds(pl.multiple_of(k * packed + i * step, step), step), :] = (
                code.astype(jnp.float32) * sc
            ).astype(jnp.bfloat16)
        return carry

    def dequant_some(part, parts):
        lax.fori_loop(part * blocks // parts, (part + 1) * blocks // parts, dequant_embed, 0)

    for part in range(lag):
        dequant_some(part, lag)
        if nf > 2:
            pass_on(1, pieces - lag + part)
    for j in range(2, nf - 2):
        for i in range(pieces):
            pass_on(j, i)

    mark("prep")
    post_row, final_row = post_gain[...].reshape(1, width_d), final_gain[...].reshape(1, width_d)
    for z in range(nf):
        post_z[z] = post_row[:, z * cols:(z + 1) * cols]
        final_z[z] = final_row[:, z * cols:(z + 1) * cols]
    side = lax.broadcasted_iota(jnp.int32, (1, 128), 1)
    entry = jnp.zeros((1, 128), jnp.int32)
    for i in range(tok):
        entry = jnp.where(side == i, targets[i], jnp.where(side == 64 + i, mask[i], entry))
    info[...] = entry
    infos[s * nf + f] = entry

    for j in range(rest):
        for way in (0, 1):
            res_send(way, j, jnp.logical_and(inner, jnp.logical_not(late(way))))

    mark("near_mm")
    swap.wait_recv()
    edge = jnp.logical_not(inner)
    near_acc = jnp.zeros((rest * 2 * tok, cols), jnp.float32)
    for i in range(pieces):
        if nf > 3:
            pass_on(nf - 2, i)
        for b in range(nf):
            @pl.when(jnp.logical_and(edge, jnp.logical_and(f != b, far != b)))
            def _():
                arrive(b, i)

        lhs = gathered[pl.ds(first, rest), i].astype(jnp.float32).reshape(
            rest * 2 * tok, piece
        ).astype(jnp.bfloat16)
        near_acc = near_acc + jnp.dot(
            lhs, weight[i * piece:(i + 1) * piece], preferred_element_type=jnp.float32
        )
    for b in range(rest):
        for h in (0, 1):
            at = (2 * b + h) * tok
            near_own[h, b * tok:(b + 1) * tok] = near_acc[at:at + tok]
    near_swap = remote(
        near_own.at[1 - s], near_in, near_sem.at[0], near_sem.at[1], f, m, 1 - s
    )
    near_swap.start()
    for way in (0, 1):
        res_send(way, 0, late(way), share(1))

    def to_peers(part, mid, sems):
        for d in range(1, nm):
            remote(
                part, mid.at[m], sems.at[0], sems.at[1], f, lax.rem(m + d, nm), s
            ).start()

    def peers(mid, sems):
        ref = mid.at[pl.ds(0, nm - 1)]
        return remote(ref, ref, sems.at[0], sems.at[1], f, m, 1 - s)

    def gather_peers(part, mid, sems):
        if nm > 1:
            peers(mid, sems).wait_recv()
        full = part[...]
        for d in range(1, nm):
            full = full + mid[lax.rem(m + d, nm)]
        return full

    def nearer(d):
        return jnp.where(low, lax.rem(f + d, nf), lax.rem(f + nf - d, nf))

    def early_sends():
        spot = infos.at[s * nf + f]
        for d in range(1, nf):
            for h in (0, 1):
                remote(info, spot, info_sem.at[0], info_sem.at[1], lax.rem(f + d, nf), m, h).start()
        remote(info, spot, info_sem.at[0], info_sem.at[1], f, m, 1 - s).start()

    gains = post_z[f] * final_z[f]
    near_at = pl.ds(first, rest)

    def near_to(z, pf, ps, send, recv):
        return remote(
            states.at[z, s, near_at], states.at[z, s, near_at], send, recv, pf, m, ps
        )

    def near_span(z):
        return pl.ds(jnp.where(z < nf - nf // 2, 0, 1), rest)

    def far_spot(z):
        return jnp.where(z < nf - nf // 2, nf - 1, 0)

    def near_states():
        near_ffn = gather_peers(near_part, near_mid, near_mp)
        ffn[pl.ds(first, rest)] = near_ffn.reshape(rest, tok, cols)
        states[f, s, near_at] = (near_ffn * gains).reshape(rest, tok, cols).astype(jnp.bfloat16)
        for d in range(rest, 0, -1):
            near_to(f, nearer(d), s, near_send, near_recv.at[f]).start()
        near_to(f, f, 1 - s, near_fwd.at[nf], near_fwd.at[f]).start()

    mark("far_mm")
    far_acc = jnp.zeros((2 * tok, cols), jnp.float32)
    reduce_at, send_at = min(1, pieces - 1), min(6, pieces - 1)
    for i in range(pieces):
        if i == pieces - 1 and i > reduce_at:
            near_states()
        @pl.when(edge)
        def _():
            arrive(far, i)

        lhs = gathered[far, i].astype(jnp.float32).reshape(2 * tok, piece).astype(jnp.bfloat16)
        far_acc = far_acc + jnp.dot(
            lhs, weight[i * piece:(i + 1) * piece], preferred_element_type=jnp.float32
        )
        if i == reduce_at:
            near_swap.wait_recv()
            near_part[...] = near_own[s] + near_in[...]
            to_peers(near_part, near_mid, near_mp)
            if pieces - 1 <= reduce_at:
                near_states()
        if i == send_at:
            early_sends()
        for j in range(1, rest):
            if i == min(4 + j, pieces - 1):
                for way in (0, 1):
                    res_send(way, j, late(way), share(j + 1))
    for h in (0, 1):
        far_own[h] = far_acc[h * tok:(h + 1) * tok]
    mark("far_swap")
    slot = far_mid.at[2 * m + s]
    for d in range(1, nm):
        for h in (0, 1):
            remote(
                far_own.at[h], slot, far_mp.at[0], far_mp.at[1], f, lax.rem(m + d, nm), h
            ).start()
    remote(far_own.at[1 - s], slot, far_mp.at[0], far_mp.at[1], f, m, 1 - s).start()
    far_mid[2 * m + s] = far_own[s]

    mark("res_x")

    def res_hand(d):
        b = nearer(d)

        @pl.when(edge)
        def _():
            res_arrive(b, share(d))
            ref = res.at[s, b, part_z]
            if halved and d < rest:
                for e in range(1, nm):
                    remote(
                        ref, ref, res_sem.at[2], res_sem.at[3], f, lax.rem(m + e, nm), s
                    ).start()
            res_pair(b, share(d))

        @pl.when(inner)
        def _():
            res_pair(b, pl.ds(0, nf))

    for d in range(1, rest):
        res_hand(d)
    mark("far_mp")
    far_all = far_mid.at[pl.ds(0, 2 * nm - 1)]
    far_sum = remote(far_all, far_all, far_mp.at[0], far_mp.at[1], f, m, 1 - s)
    far_sum.wait_recv()
    far_ffn = jnp.sum(far_mid[...], axis=0)
    ffn[far] = far_ffn
    states[f, s, far] = (far_ffn * gains).astype(jnp.bfloat16)

    mine_far = states.at[f, s, far]
    for d in range(rest, 0, -1):
        for h in (0, 1):
            remote(mine_far, mine_far, far_send, far_recv.at[f], nearer(d), m, h).start()
    remote(mine_far, mine_far, far_send, far_recv.at[f], f, m, 1 - s).start()

    mark("moments")
    mine = nf * tok
    y = ffn[...].reshape(mine, cols)
    g = y * post_z[f]
    lane = lax.broadcasted_iota(jnp.int32, (mine, 128), 1)

    def row_sum(v):
        return jnp.sum(v, axis=1, keepdims=True)

    def tall(v):
        extra = 128 - v.shape[0]
        return v if extra == 0 else jnp.concatenate([v, jnp.zeros((extra, 128), jnp.float32)], axis=0)

    moments[2 * f + s] = jnp.transpose(tall(jnp.where(lane < 1, row_sum(y * y), row_sum(g * g))))[0:8]
    mine_mom = moments.at[2 * f + s]
    for d in range(rest, 0, -1):
        for h in (0, 1):
            remote(mine_mom, mine_mom, mom_sem.at[0], mom_sem.at[1], nearer(d), m, h).start()
    remote(mine_mom, mine_mom, mom_sem.at[0], mom_sem.at[1], f, m, 1 - s).start()

    def same(z, span, sems, recv):
        ref = states.at[z, s, span]
        return remote(ref, ref, sems, recv, f, m, 1 - s)

    def other(z, span, sems, recv):
        ref = states.at[z, 1 - s, span]
        return remote(ref, ref, sems, recv, f, m, 1 - s)

    def hand_near(d):
        z = nearer(d)
        same(z, near_span(z), near_send, near_recv.at[z]).wait_recv()
        same(z, near_span(z), near_fwd.at[nf], near_fwd.at[z]).start()

    def crossed(d):
        z = nearer(d)
        return row_sum(states[z].astype(jnp.float32).reshape(total, cols) * ratio[z])

    def product(d):
        z = nearer(d)
        other(z, near_span(z), near_fwd.at[nf], near_fwd.at[z]).wait_recv()
        ref = states.at[z, 1 - s, far_spot(z)] if d == 0 else states.at[z, :, far_spot(z)]
        remote(ref, ref, far_send, far_recv.at[z], f, m, 1 - s).wait_recv()
        wide = states[z].astype(jnp.float32).reshape(total, cols)
        return jnp.dot(
            wide.astype(jnp.bfloat16), embed[pl.ds(pl.multiple_of(z * cols, 32), cols), :],
            preferred_element_type=jnp.float32,
        )

    mark("info")
    info_all = infos.at[pl.ds(0, 2 * nf - 1)]
    info_in = remote(info_all, info_all, info_sem.at[0], info_sem.at[1], f, m, 1 - s)
    info_in.wait_recv()
    turned = jnp.transpose(tall(infos[...].astype(jnp.float32).reshape(2 * nf, 128)))
    wanted = jnp.concatenate([turned[0:tok, e:e + 1] for e in range(2 * nf)], axis=0).astype(jnp.int32)
    counted = jnp.concatenate([turned[64:64 + tok, e:e + 1] for e in range(2 * nf)], axis=0)
    weights = jnp.transpose(
        jnp.concatenate(
            [jnp.broadcast_to(counted, (total, 128)), jnp.zeros((total, 128), jnp.float32)], axis=0
        )
    )[0:1, :]

    mark("res_wait")
    res_hand(rest)
    rest_ref = res.at[s, pl.ds(0, max(rest - 1, 1)), pl.ds(0, max(nf - span_z, 1))]
    res_x = remote(rest_ref, rest_ref, res_sem.at[2], res_sem.at[3], f, m, 1 - s)
    if halved and nm > 1:
        @pl.when(edge)
        def _():
            res_x.wait_recv()
            for d in range(1, rest):
                for e in range(1, nm):
                    res_pair(nearer(d), pl.ds(lax.rem(m + e, nm) * span_z, span_z))

    res_in = remote(res.at[1 - s], res.at[1 - s], res_sem.at[0], res_sem.at[1], f, m, 1 - s)
    def residual_product():
        res_in.wait_recv()
        power = jnp.zeros((total, 1), jnp.float32)
        base = jnp.zeros((2 * total, vocab), jnp.float32)
        for z in range(nf):
            rz = res[:, :, z].astype(jnp.float32).reshape(total, cols)
            power = power + row_sum(rz * rz)
            ratio[z] = rz / final_z[z]
            rf = rz * final_z[z]
            high = rf.astype(jnp.bfloat16)
            low_part = (rf - high.astype(jnp.float32)).astype(jnp.bfloat16)
            base = base + jnp.dot(
                jnp.concatenate([high, low_part], axis=0), embed[z * cols:(z + 1) * cols],
                preferred_element_type=jnp.float32,
            )
        base_sum[...] = base[0:total] + base[total:]
        power_sum[...] = jnp.broadcast_to(power, (total, 128))

    mark("logits0a")

    @pl.when(inner)
    def _():
        residual_product()

    mark("near_fwd1")
    for d in range(1, rest):
        hand_near(d)
    hand_near(rest)
    mark("product0")
    main = product(0)
    mark("logits0b")

    @pl.when(edge)
    def _():
        residual_product()

    base, power = base_sum[...], power_sum[:, 0:1]
    cross = crossed(0)

    mark("logits1")
    for d in range(1, rest):
        main, cross = main + product(d), cross + crossed(d)
    mark("last")
    mom_all = moments.at[pl.ds(0, 2 * nf - 1)]
    mom_in = remote(mom_all, mom_all, mom_sem.at[0], mom_sem.at[1], f, m, 1 - s)
    mom_in.wait_recv()
    turned = jnp.transpose(tall(
        jnp.sum(moments[...].reshape(nf, 2, 8, 128), axis=0).reshape(16, 128)
    ))

    def column(q):
        return jnp.concatenate([turned[0:mine, q:q + 1], turned[0:mine, q + 8:q + 9]], axis=0)

    inv = lax.rsqrt(column(0) / width_d + EPS)
    square = power + inv * inv * column(1)
    mark("logits2")
    main, cross = main + product(rest), cross + crossed(rest)
    inv2 = lax.rsqrt((square + 2.0 * inv * cross) / width_d + EPS)
    logits = (base + main * inv) * inv2
    capped = CAP * jnp.tanh(logits / CAP)
    ids = me * vocab + lax.broadcasted_iota(jnp.int32, (total, vocab), 1)
    hits = wanted == ids
    e = jnp.sum(jnp.exp(capped), axis=1, keepdims=True)
    t = jnp.sum(jnp.where(hits, capped, 0.0), axis=1, keepdims=True)
    both = jnp.concatenate(
        [jnp.broadcast_to(e, (total, 128)), jnp.broadcast_to(t, (total, 128))], axis=0
    )
    sums[me] = jnp.transpose(both)[0:1, :]
    mark("sums")
    for d in range(1, n):
        pf, pm, ps = where_is(lax.rem(me + d, n))
        remote(sums.at[me], sums.at[me], sum_sem.at[0], sum_sem.at[1], pf, pm, ps).start()
    sum_all = sums.at[pl.ds(0, n - 1)]
    sum_in = remote(sum_all, sum_all, sum_sem.at[0], sum_sem.at[1], f, m, 1 - s)
    sum_in.wait_recv()
    mark("final")
    added = jnp.sum(sums[...], axis=0)
    pad = 2 * total
    spot = lax.broadcasted_iota(jnp.int32, (1, pad), 1)
    exp_sums = jnp.where(spot < total, added, 1.0)
    losses = weights * (jnp.log(exp_sums) - pltpu.roll(added, total, 1))
    mean = jnp.sum(losses, axis=1, keepdims=True) / jnp.maximum(
        jnp.sum(weights, axis=1, keepdims=True), 1.0
    )
    start = (s * nf + f) * tok
    mine_out = pltpu.roll(losses, lax.rem(pad - start, pad), 1)
    out[...] = jnp.where(spot < tok, mine_out, mean)[0, 0:out.shape[0]]

    mark("drain")
    for way in (0, 1):
        for j in range(1, nf):
            going = has_up if way == 0 else has_down

            @pl.when(jnp.logical_and(going, held(way, j - 1)))
            def _():
                remote(
                    gathered.at[0], gathered.at[0], hid_send.at[way, j - 1], hid_recv.at[0, 0], f, m, 1 - s
                ).wait_send()
    swap.wait_send()
    near_swap.wait_send()
    far_sum.wait_send()
    if nm > 1:
        peers(near_mid, near_mp).wait_send()
    for way in (0, 1):
        for j in range(rest):
            going = jnp.logical_and(has_up if way == 0 else has_down, held(way, j))
            for zs, when in ((share(j + 1), late(way)), (whole_z, jnp.logical_not(late(way)))):
                @pl.when(jnp.logical_and(going, when))
                def _():
                    ref = res.at[s, 0, zs]
                    remote(
                        ref, ref, res_sem.at[4 + way * nf + j], res_recv.at[0], f, m, 1 - s
                    ).wait_send()

    res_in.wait_send()
    if halved and nm > 1:
        @pl.when(edge)
        def _():
            res_x.wait_send()

    info_in.wait_send()
    mom_in.wait_send()
    near_all = states.at[pl.ds(0, rest), 0, pl.ds(0, rest)]
    remote(near_all, near_all, near_send, near_recv.at[0], f, m, 1 - s).wait_send()
    for h in (0, 1):
        far_all = states.at[pl.ds(0, nf - h), 0, 0]
        remote(far_all, far_all, far_send, far_recv.at[0], f, m, 1 - s).wait_send()
    near_all = states.at[:, 0, pl.ds(0, rest)]
    remote(near_all, near_all, near_fwd.at[nf], near_fwd.at[0], f, m, 1 - s).wait_send()
    sum_in.wait_send()
    mark(None)


def finish(tok, row, losses, mean):
    losses[...] = row[0:tok]
    mean[...] = row[tok:tok + 1]


def on_device(
    nf, nm, hidden, residual, down_packed, down_scale, post_gain, final_gain, embed_packed, embed_scale,
    targets, loss_mask,
):
    tok, width_d = residual.shape
    rows, cols = down_packed.shape
    vocab, packed = embed_packed.shape
    half = rows // 2
    half_k = half * PLANES
    n = nf * nm * 2
    total = tok * 2 * nf
    rest = nf - 1
    groups = half_k // GROUP
    pieces = next(c for c in PIECES if groups % c == 0 and half_k // c % 256 == 0 or c == 1)
    piece = half_k // pieces
    width = 256 if piece % 256 == 0 else GROUP
    vm = pl.BlockSpec(memory_space=pltpu.VMEM)
    hbm = pl.BlockSpec(memory_space=pltpu.HBM)
    dma = pltpu.SemaphoreType.DMA
    bf16, f32, i32 = jnp.bfloat16, jnp.float32, jnp.int32
    row = pl.pallas_call(
        functools.partial(kernel, nf, nm),
        out_shape=jax.ShapeDtypeStruct((128,), f32),
        in_specs=[hbm] * 10,
        out_specs=vm,
        scratch_shapes=[
            pltpu.VMEM(hidden.shape, bf16),
            pltpu.VMEM(residual.shape, bf16),
            pltpu.VMEM((half, cols), i32),
            pltpu.VMEM(down_scale.shape, bf16),
            pltpu.VMEM((width_d,), f32),
            pltpu.VMEM((width_d,), f32),
            pltpu.VMEM((packed, vocab), i32),
            pltpu.VMEM((embed_scale.shape[1], vocab), bf16),
            pltpu.SMEM((tok,), i32),
            pltpu.SMEM((tok,), i32),
            pltpu.VMEM(down_scale.shape, f32),
            pltpu.VMEM((embed_scale.shape[1], vocab), f32),
            pltpu.VMEM((nf, 1, cols), f32),
            pltpu.VMEM((nf, 1, cols), f32),
            pltpu.VMEM((half_k, cols), bf16),
            pltpu.VMEM((width_d, vocab), bf16),
            pltpu.VMEM((width, width), bf16),
            pltpu.VMEM((2, pieces, tok, piece), bf16),
            pltpu.VMEM((nf, pieces, 2, tok, piece), bf16),
            pltpu.VMEM((2, rest * tok, cols), f32),
            pltpu.VMEM((rest * tok, cols), f32),
            pltpu.VMEM((rest * tok, cols), f32),
            pltpu.VMEM((nm, rest * tok, cols), f32),
            pltpu.VMEM((2, tok, cols), f32),
            pltpu.VMEM((2 * nm, tok, cols), f32),
            pltpu.VMEM((nf, tok, cols), f32),
            pltpu.VMEM((2, nf, nf, tok, cols), bf16),
            pltpu.VMEM((nf, 2, nf, tok, cols), bf16),
            pltpu.VMEM((2 * nf, 8, 128), f32),
            pltpu.VMEM((nf, total, cols), f32),
            pltpu.VMEM((total, vocab), f32),
            pltpu.VMEM((total, 128), f32),
            pltpu.VMEM((1, 128), i32),
            pltpu.VMEM((2 * nf, 1, 128), i32),
            pltpu.VMEM((n, 1, 2 * total), f32),
            dma((10,)),
            dma((2, max(nf - 1, 1))), dma((nf, pieces)),
            dma((2,)), dma((2,)), dma((2,)), dma((2,)),
            dma((4 + 2 * nf,)), dma((nf,)), dma((2,)),
            dma, dma((nf,)), dma, dma((nf,)), dma((nf + 1,)),
            dma((2,)), dma((2,)),
        ],
        compiler_params=pltpu.CompilerParams(
            collective_id=0, has_side_effects=True, vmem_limit_bytes=60 * 1024 * 1024
        ),
    )(
        hidden, residual, down_packed, down_scale, post_gain, final_gain,
        embed_packed.T, embed_scale.T, targets, loss_mask,
    )
    return pl.pallas_call(
        functools.partial(finish, tok),
        out_shape=(jax.ShapeDtypeStruct((tok,), f32), jax.ShapeDtypeStruct((1,), f32)),
        in_specs=[vm],
        out_specs=(vm, vm),
    )(row)


def solution(mesh):
    nf, nm = mesh.shape["fsdp"], mesh.shape["mp"]
    return jax.shard_map(
        functools.partial(on_device, nf, nm),
        mesh=mesh,
        in_specs=(
            P(("groups", "fsdp", "sub"), "mp"),
            P(("groups", "fsdp", "sub"), None),
            P("mp", "fsdp"),
            P("mp", "fsdp"),
            P(),
            P(),
            P(("fsdp", "mp", "sub"), None),
            P(("fsdp", "mp", "sub"), None),
            P(("groups", "fsdp", "sub")),
            P(("groups", "fsdp", "sub")),
        ),
        out_specs=(P(("groups", "fsdp", "sub")), P("groups")),
        check_vma=False,
    )
```

```python
import functools

import jax
import jax.numpy as jnp
from jax import lax
from jax.experimental import pallas as pl
from jax.experimental.pallas import tpu as pltpu
from jax.sharding import PartitionSpec as P

EPS = 1e-06
CAP = 30.0
MESH = pl.DeviceIdType.MESH
PLANES = 8
GROUP = 128
PIECES = (9, 8, 6, 4, 3, 2, 1)


def remote(src, dst, send, recv, f, m, s):
    return pltpu.make_async_remote_copy(
        src_ref=src,
        dst_ref=dst,
        send_sem=send,
        recv_sem=recv,
        device_id={"fsdp": f, "mp": m, "sub": s},
        device_id_type=MESH,
    )


def mark(name):
    pass


def kernel(
    nf, nm, hidden_hbm, residual_hbm, words_hbm, scale_hbm, post_hbm, final_hbm, embed_hbm, embed_scale_hbm,
    targets_hbm, mask_hbm,
    out,
    hidden, residual, words, scale, post_gain, final_gain, embed_words, embed_scale, targets, mask,
    scale_f, embed_f, post_z, final_z, weight, embed, perm, sorted_own, gathered,
    near_own, near_in, near_part, near_mid, far_own, far_mid,
    ffn, res, states, moments, ratio, base_sum, power_sum, info, infos, sums,
    local_sem, hid_send, hid_recv, pair_sem, near_sem, near_mp, far_mp, res_sem, res_recv, info_sem,
    near_send, near_recv, far_send, far_recv, near_fwd, mom_sem, sum_sem,
):
    f, m, s = lax.axis_index("fsdp"), lax.axis_index("mp"), lax.axis_index("sub")
    n = nf * nm * 2
    me = (f * nm + m) * 2 + s
    tok = hidden.shape[0]
    half_rows, cols = words.shape
    half_k = half_rows * PLANES
    total = tok * 2 * nf
    width_d = nf * cols
    pieces, piece = gathered.shape[1], gathered.shape[4]
    groups = half_k // GROUP
    per = GROUP // PLANES
    rest = nf - 1
    low = f < nf - nf // 2
    far = jnp.where(low, nf - 1, 0)
    first = jnp.where(low, 0, 1)
    up, down = lax.rem(f + 1, nf), lax.rem(f + nf - 1, nf)
    has_up, has_down = f < nf - 1, f > 0
    inner = jnp.logical_and(has_up, has_down)

    def where_is(q):
        return q // (2 * nm), (q // 2) % nm, q % 2

    barrier = pltpu.get_barrier_semaphore()

    def greet(pf, pm, ps):
        pl.semaphore_signal(
            barrier, inc=1, device_id={"fsdp": pf, "mp": pm, "sub": ps}, device_id_type=MESH
        )

    @pl.when(has_up)
    def _():
        greet(up, m, 0)
        greet(up, m, 1)

    @pl.when(has_down)
    def _():
        greet(down, m, 0)
        greet(down, m, 1)

    greet(f, m, 1 - s)
    for d in range(1, nm):
        greet(f, lax.rem(m + d, nm), s)

    def load(i, src, dst):
        copy = pltpu.make_async_copy(src, dst, local_sem.at[i])
        copy.start()
        return copy

    load_hidden = load(0, hidden_hbm, hidden)
    load_residual = load(5, residual_hbm, residual)
    load_words = load(
        1, words_hbm.at[pl.ds(pl.multiple_of(s * half_rows, 8), half_rows)], words
    )
    load_scale = load(2, scale_hbm, scale)
    loads = [
        load(3, embed_hbm, embed_words), load(4, embed_scale_hbm, embed_scale),
        load(6, post_hbm, post_gain), load(7, final_hbm, final_gain),
        load(8, targets_hbm, targets), load(9, mask_hbm, mask),
    ]

    width = perm.shape[0]
    row = lax.broadcasted_iota(jnp.int32, (width, width), 0)
    col = lax.broadcasted_iota(jnp.int32, (width, width), 1)
    inside = jnp.bitwise_and(col, GROUP - 1)
    source = (col - inside) + jnp.bitwise_and(inside, per - 1) * PLANES + jnp.right_shift(inside, 4)
    perm[...] = jnp.where(row == source, 1.0, 0.0).astype(jnp.bfloat16)

    mark("hidden_wait")
    load_hidden.wait()
    mark("permute")
    own = hidden[...].astype(jnp.float32)
    spans = 2 * half_k // width
    stacked = jnp.concatenate(
        [own[:, c * width:(c + 1) * width] for c in range(spans)], axis=0
    ).astype(jnp.bfloat16)
    ordered = jnp.dot(stacked, perm[...], preferred_element_type=jnp.float32)
    for c in range(spans):
        h, at = c * width // half_k, c * width % half_k
        sorted_own[h, at // piece, :, at % piece:at % piece + width] = ordered[
            c * tok:(c + 1) * tok
        ].astype(jnp.bfloat16)

    mark("barrier")
    count = 1 + (nm - 1) + 2 * has_up.astype(jnp.int32) + 2 * has_down.astype(jnp.int32)
    pl.semaphore_wait(barrier, count)
    mark("send1")

    def first_hop(way, i):
        target = up if way == 0 else down
        for h in (0, 1):
            remote(
                sorted_own.at[h, i], gathered.at[f, i, s], hid_send.at[way, 0], hid_recv.at[f, i],
                target, m, h,
            ).start()

    def block_at(way, j):
        return lax.rem(f - j + nf, nf) if way == 0 else lax.rem(f + j, nf)

    def held(way, j):
        return f >= j if way == 0 else f + j <= nf - 1

    def arrive(b, i):
        remote(
            gathered.at[b, i], gathered.at[b, i], hid_send.at[0, 0], hid_recv.at[b, i], f, m, 1 - s
        ).wait_recv()

    def pass_on(j, i):
        for way in (0, 1):
            b = block_at(way, j)
            target = up if way == 0 else down

            @pl.when(jnp.logical_and(inner, held(way, j)))
            def _():
                arrive(b, i)
                remote(
                    gathered.at[b, i], gathered.at[b, i], hid_send.at[way, j], hid_recv.at[b, i],
                    target, m, s,
                ).start()

    for i in range(pieces):
        @pl.when(has_up)
        def _():
            first_hop(0, i)

        @pl.when(has_down)
        def _():
            first_hop(1, i)

    swap = remote(
        sorted_own.at[1 - s], gathered.at[f, :, s], pair_sem.at[0], pair_sem.at[1], f, m, 1 - s
    )
    swap.start()
    gathered[f, :, s] = sorted_own[s]
    load_residual.wait()
    own_res = residual[...].astype(jnp.float32)
    for z in range(nf):
        res[s, f, z] = own_res[:, z * cols:(z + 1) * cols].astype(jnp.bfloat16)

    halved = nf > 2 and nf % nm == 0
    span_z = nf // nm if halved else nf
    whole_z = pl.ds(0, nf)
    part_z = pl.ds(m * span_z, span_z) if halved else whole_z

    def share(d):
        return part_z if d < rest else whole_z

    def late(way):
        return jnp.logical_and(inner, (f == nf - 2) if way == 0 else (f == 1))

    def res_arrive(b, zs):
        ref = res.at[s, b, zs]
        remote(ref, ref, res_sem.at[0], res_recv.at[b], f, m, 1 - s).wait_recv()

    def res_send(way, j, when, zs=pl.ds(0, nf)):
        b = block_at(way, j)
        going = has_up if way == 0 else has_down

        @pl.when(jnp.logical_and(jnp.logical_and(going, held(way, j)), when))
        def _():
            if j > 0:
                res_arrive(b, pl.ds(0, nf))
            ref = res.at[s, b, zs]
            remote(
                ref, ref, res_sem.at[4 + way * nf + j], res_recv.at[b], up if way == 0 else down, m, s
            ).start()

    def res_pair(b, zs):
        ref = res.at[s, b, zs]
        remote(ref, ref, res_sem.at[0], res_sem.at[1], f, m, 1 - s).start()

    for way in (0, 1):
        res_send(way, 0, jnp.logical_not(inner))
    res_pair(f, pl.ds(0, nf))

    mark("deq")
    load_scale.wait()
    scale_f[...] = scale[...].astype(jnp.float32)
    load_words.wait()

    def dequant(g, carry):
        w = words[pl.ds(pl.multiple_of(g * per, per), per), :]
        sc = scale_f[pl.ds(s * groups + g, 1), :]
        for k in range(PLANES):
            code = jnp.right_shift(jnp.left_shift(w, 28 - 4 * k), 28) if k < 7 else jnp.right_shift(w, 28)
            weight[pl.ds(pl.multiple_of(g * GROUP + k * per, per), per), :] = (
                code.astype(jnp.float32) * sc
            ).astype(jnp.bfloat16)
        return carry

    each = groups // pieces
    lag = min(3, pieces)
    for i in range(pieces):
        lax.fori_loop(i * each, (i + 1) * each, dequant, 0)
        if i >= lag and nf > 2:
            pass_on(1, i - lag)

    mark("deqE")
    for copy in loads:
        copy.wait()
    embed_f[...] = embed_scale[...].astype(jnp.float32)
    packed, vocab = embed_words.shape
    span = packed * PLANES // embed_f.shape[0]
    step = 32
    blocks = packed // step

    def dequant_embed(i, carry):
        w = embed_words[pl.ds(pl.multiple_of(i * step, step), step), :]
        for k in range(PLANES):
            code = jnp.right_shift(jnp.left_shift(w, 28 - 4 * k), 28) if k < 7 else jnp.right_shift(w, 28)
            sc = embed_f[pl.ds((k * packed + i * step) // span, 1), :]
            embed[pl.ds(pl.multiple_of(k * packed + i * step, step), step), :] = (
                code.astype(jnp.float32) * sc
            ).astype(jnp.bfloat16)
        return carry

    def dequant_some(part, parts):
        lax.fori_loop(part * blocks // parts, (part + 1) * blocks // parts, dequant_embed, 0)

    for part in range(lag):
        dequant_some(part, lag)
        if nf > 2:
            pass_on(1, pieces - lag + part)
    for j in range(2, nf - 2):
        for i in range(pieces):
            pass_on(j, i)

    mark("prep")
    post_row, final_row = post_gain[...].reshape(1, width_d), final_gain[...].reshape(1, width_d)
    for z in range(nf):
        post_z[z] = post_row[:, z * cols:(z + 1) * cols]
        final_z[z] = final_row[:, z * cols:(z + 1) * cols]
    side = lax.broadcasted_iota(jnp.int32, (1, 128), 1)
    entry = jnp.zeros((1, 128), jnp.int32)
    for i in range(tok):
        entry = jnp.where(side == i, targets[i], jnp.where(side == 64 + i, mask[i], entry))
    info[...] = entry
    infos[s * nf + f] = entry

    for j in range(rest):
        for way in (0, 1):
            res_send(way, j, jnp.logical_and(inner, jnp.logical_not(late(way))))

    mark("near_mm")
    swap.wait_recv()
    edge = jnp.logical_not(inner)
    near_acc = jnp.zeros((rest * 2 * tok, cols), jnp.float32)
    for i in range(pieces):
        if nf > 3:
            pass_on(nf - 2, i)
        for b in range(nf):
            @pl.when(jnp.logical_and(edge, jnp.logical_and(f != b, far != b)))
            def _():
                arrive(b, i)

        lhs = gathered[pl.ds(first, rest), i].astype(jnp.float32).reshape(
            rest * 2 * tok, piece
        ).astype(jnp.bfloat16)
        near_acc = near_acc + jnp.dot(
            lhs, weight[i * piece:(i + 1) * piece], preferred_element_type=jnp.float32
        )
    for b in range(rest):
        for h in (0, 1):
            at = (2 * b + h) * tok
            near_own[h, b * tok:(b + 1) * tok] = near_acc[at:at + tok]
    near_swap = remote(
        near_own.at[1 - s], near_in, near_sem.at[0], near_sem.at[1], f, m, 1 - s
    )
    near_swap.start()
    for way in (0, 1):
        res_send(way, 0, late(way), share(1))

    def to_peers(part, mid, sems):
        for d in range(1, nm):
            remote(
                part, mid.at[m], sems.at[0], sems.at[1], f, lax.rem(m + d, nm), s
            ).start()

    def peers(mid, sems):
        ref = mid.at[pl.ds(0, nm - 1)]
        return remote(ref, ref, sems.at[0], sems.at[1], f, m, 1 - s)

    def gather_peers(part, mid, sems):
        if nm > 1:
            peers(mid, sems).wait_recv()
        full = part[...]
        for d in range(1, nm):
            full = full + mid[lax.rem(m + d, nm)]
        return full

    def nearer(d):
        return jnp.where(low, lax.rem(f + d, nf), lax.rem(f + nf - d, nf))

    def early_sends():
        spot = infos.at[s * nf + f]
        for d in range(1, nf):
            for h in (0, 1):
                remote(info, spot, info_sem.at[0], info_sem.at[1], lax.rem(f + d, nf), m, h).start()
        remote(info, spot, info_sem.at[0], info_sem.at[1], f, m, 1 - s).start()

    gains = post_z[f] * final_z[f]
    near_at = pl.ds(first, rest)

    def near_to(z, pf, ps, send, recv):
        return remote(
            states.at[z, s, near_at], states.at[z, s, near_at], send, recv, pf, m, ps
        )

    def near_span(z):
        return pl.ds(jnp.where(z < nf - nf // 2, 0, 1), rest)

    def far_spot(z):
        return jnp.where(z < nf - nf // 2, nf - 1, 0)

    def near_states():
        near_ffn = gather_peers(near_part, near_mid, near_mp)
        ffn[pl.ds(first, rest)] = near_ffn.reshape(rest, tok, cols)
        states[f, s, near_at] = (near_ffn * gains).reshape(rest, tok, cols).astype(jnp.bfloat16)
        for d in range(rest, 0, -1):
            near_to(f, nearer(d), s, near_send, near_recv.at[f]).start()
        near_to(f, f, 1 - s, near_fwd.at[nf], near_fwd.at[f]).start()

    mark("far_mm")
    far_acc = jnp.zeros((2 * tok, cols), jnp.float32)
    reduce_at, send_at = min(1, pieces - 1), min(6, pieces - 1)
    for i in range(pieces):
        if i == pieces - 1 and i > reduce_at:
            near_states()
        @pl.when(edge)
        def _():
            arrive(far, i)

        lhs = gathered[far, i].astype(jnp.float32).reshape(2 * tok, piece).astype(jnp.bfloat16)
        far_acc = far_acc + jnp.dot(
            lhs, weight[i * piece:(i + 1) * piece], preferred_element_type=jnp.float32
        )
        if i == reduce_at:
            near_swap.wait_recv()
            near_part[...] = near_own[s] + near_in[...]
            to_peers(near_part, near_mid, near_mp)
            if pieces - 1 <= reduce_at:
                near_states()
        if i == send_at:
            early_sends()
        for j in range(1, rest):
            if i == min(4 + j, pieces - 1):
                for way in (0, 1):
                    res_send(way, j, late(way), share(j + 1))
    for h in (0, 1):
        far_own[h] = far_acc[h * tok:(h + 1) * tok]
    mark("far_swap")
    slot = far_mid.at[2 * m + s]
    for d in range(1, nm):
        for h in (0, 1):
            remote(
                far_own.at[h], slot, far_mp.at[0], far_mp.at[1], f, lax.rem(m + d, nm), h
            ).start()
    remote(far_own.at[1 - s], slot, far_mp.at[0], far_mp.at[1], f, m, 1 - s).start()
    far_mid[2 * m + s] = far_own[s]

    mark("res_x")

    def res_hand(d):
        b = nearer(d)

        @pl.when(edge)
        def _():
            res_arrive(b, share(d))
            ref = res.at[s, b, part_z]
            if halved and d < rest:
                for e in range(1, nm):
                    remote(
                        ref, ref, res_sem.at[2], res_sem.at[3], f, lax.rem(m + e, nm), s
                    ).start()
            res_pair(b, share(d))

        @pl.when(inner)
        def _():
            res_pair(b, pl.ds(0, nf))

    for d in range(1, rest):
        res_hand(d)
    mark("far_mp")
    far_all = far_mid.at[pl.ds(0, 2 * nm - 1)]
    far_sum = remote(far_all, far_all, far_mp.at[0], far_mp.at[1], f, m, 1 - s)
    far_sum.wait_recv()
    far_ffn = jnp.sum(far_mid[...], axis=0)
    ffn[far] = far_ffn
    states[f, s, far] = (far_ffn * gains).astype(jnp.bfloat16)

    mine_far = states.at[f, s, far]
    for d in range(rest, 0, -1):
        for h in (0, 1):
            remote(mine_far, mine_far, far_send, far_recv.at[f], nearer(d), m, h).start()
    remote(mine_far, mine_far, far_send, far_recv.at[f], f, m, 1 - s).start()

    mark("moments")
    mine = nf * tok
    y = ffn[...].reshape(mine, cols)
    g = y * post_z[f]
    lane = lax.broadcasted_iota(jnp.int32, (mine, 128), 1)

    def row_sum(v):
        return jnp.sum(v, axis=1, keepdims=True)

    def tall(v):
        extra = 128 - v.shape[0]
        return v if extra == 0 else jnp.concatenate([v, jnp.zeros((extra, 128), jnp.float32)], axis=0)

    both_rows = jnp.transpose(tall(jnp.where(lane < 1, row_sum(y * y), row_sum(g * g))))
    moments[2 * f + s] = jnp.concatenate([both_rows[0:1], both_rows[1:2]], axis=1)
    mine_mom = moments.at[2 * f + s]
    for d in range(rest, 0, -1):
        for h in (0, 1):
            remote(mine_mom, mine_mom, mom_sem.at[0], mom_sem.at[1], nearer(d), m, h).start()
    remote(mine_mom, mine_mom, mom_sem.at[0], mom_sem.at[1], f, m, 1 - s).start()

    def same(z, span, sems, recv):
        ref = states.at[z, s, span]
        return remote(ref, ref, sems, recv, f, m, 1 - s)

    def other(z, span, sems, recv):
        ref = states.at[z, 1 - s, span]
        return remote(ref, ref, sems, recv, f, m, 1 - s)

    def hand_near(d):
        z = nearer(d)
        same(z, near_span(z), near_send, near_recv.at[z]).wait_recv()
        same(z, near_span(z), near_fwd.at[nf], near_fwd.at[z]).start()

    def crossed(d):
        z = nearer(d)
        return row_sum(states[z].astype(jnp.float32).reshape(total, cols) * ratio[z])

    def product(d):
        z = nearer(d)
        other(z, near_span(z), near_fwd.at[nf], near_fwd.at[z]).wait_recv()
        ref = states.at[z, 1 - s, far_spot(z)] if d == 0 else states.at[z, :, far_spot(z)]
        remote(ref, ref, far_send, far_recv.at[z], f, m, 1 - s).wait_recv()
        wide = states[z].astype(jnp.float32).reshape(total, cols)
        return jnp.dot(
            wide.astype(jnp.bfloat16), embed[pl.ds(pl.multiple_of(z * cols, 32), cols), :],
            preferred_element_type=jnp.float32,
        )

    mark("info")
    info_all = infos.at[pl.ds(0, 2 * nf - 1)]
    info_in = remote(info_all, info_all, info_sem.at[0], info_sem.at[1], f, m, 1 - s)
    info_in.wait_recv()
    turned = jnp.transpose(tall(infos[...].astype(jnp.float32).reshape(2 * nf, 128)))
    wanted = jnp.concatenate([turned[0:tok, e:e + 1] for e in range(2 * nf)], axis=0).astype(jnp.int32)
    counted = jnp.concatenate([turned[64:64 + tok, e:e + 1] for e in range(2 * nf)], axis=0)
    weights = jnp.transpose(
        jnp.concatenate(
            [jnp.broadcast_to(counted, (total, 128)), jnp.zeros((total, 128), jnp.float32)], axis=0
        )
    )[0:1, :]

    mark("res_wait")
    res_hand(rest)
    rest_ref = res.at[s, pl.ds(0, max(rest - 1, 1)), pl.ds(0, max(nf - span_z, 1))]
    res_x = remote(rest_ref, rest_ref, res_sem.at[2], res_sem.at[3], f, m, 1 - s)
    if halved and nm > 1:
        @pl.when(edge)
        def _():
            res_x.wait_recv()
            for d in range(1, rest):
                for e in range(1, nm):
                    res_pair(nearer(d), pl.ds(lax.rem(m + e, nm) * span_z, span_z))

    res_in = remote(res.at[1 - s], res.at[1 - s], res_sem.at[0], res_sem.at[1], f, m, 1 - s)
    def residual_product():
        res_in.wait_recv()
        power = jnp.zeros((total, 1), jnp.float32)
        base = jnp.zeros((2 * total, vocab), jnp.float32)
        for z in range(nf):
            rz = res[:, :, z].astype(jnp.float32).reshape(total, cols)
            power = power + row_sum(rz * rz)
            ratio[z] = rz / final_z[z]
            rf = rz * final_z[z]
            high = rf.astype(jnp.bfloat16)
            low_part = (rf - high.astype(jnp.float32)).astype(jnp.bfloat16)
            base = base + jnp.dot(
                jnp.concatenate([high, low_part], axis=0), embed[z * cols:(z + 1) * cols],
                preferred_element_type=jnp.float32,
            )
        base_sum[...] = base[0:total] + base[total:]
        power_sum[...] = jnp.broadcast_to(power, (total, 128))

    mark("logits0a")

    @pl.when(inner)
    def _():
        residual_product()

    mark("near_fwd1")
    for d in range(1, rest):
        hand_near(d)
    hand_near(rest)
    mark("product0")
    main = product(0)
    mark("logits0b")

    @pl.when(edge)
    def _():
        residual_product()

    base, power = base_sum[...], power_sum[:, 0:1]
    cross = crossed(0)

    mark("logits1")
    for d in range(1, rest):
        main, cross = main + product(d), cross + crossed(d)
    mark("last")
    mom_all = moments.at[pl.ds(0, 2 * nf - 1)]
    mom_in = remote(mom_all, mom_all, mom_sem.at[0], mom_sem.at[1], f, m, 1 - s)
    mom_in.wait_recv()
    halves = [
        functools.reduce(jnp.add, [moments[2 * z + h] for z in range(nf)]) for h in (0, 1)
    ]
    turned = jnp.transpose(tall(jnp.concatenate(
        [half[:, k:k + 128] for k in (0, 128) for half in halves], axis=0
    )))

    def column(q):
        return jnp.concatenate([turned[0:mine, 2 * q:2 * q + 1], turned[0:mine, 2 * q + 1:2 * q + 2]], axis=0)

    inv = lax.rsqrt(column(0) / width_d + EPS)
    square = power + inv * inv * column(1)
    mark("logits2")
    main, cross = main + product(rest), cross + crossed(rest)
    inv2 = lax.rsqrt((square + 2.0 * inv * cross) / width_d + EPS)
    logits = (base + main * inv) * inv2
    capped = CAP * jnp.tanh(logits / CAP)
    ids = me * vocab + lax.broadcasted_iota(jnp.int32, (total, vocab), 1)
    hits = wanted == ids
    e = jnp.sum(jnp.exp(capped), axis=1, keepdims=True)
    t = jnp.sum(jnp.where(hits, capped, 0.0), axis=1, keepdims=True)
    both = jnp.concatenate(
        [jnp.broadcast_to(e, (total, 128)), jnp.broadcast_to(t, (total, 128))], axis=0
    )
    sums[me] = jnp.transpose(both)[0:1, :]
    mark("sums")
    for d in range(1, n):
        pf, pm, ps = where_is(lax.rem(me + d, n))
        remote(sums.at[me], sums.at[me], sum_sem.at[0], sum_sem.at[1], pf, pm, ps).start()
    sum_all = sums.at[pl.ds(0, n - 1)]
    sum_in = remote(sum_all, sum_all, sum_sem.at[0], sum_sem.at[1], f, m, 1 - s)
    sum_in.wait_recv()
    mark("final")
    added = jnp.sum(sums[...], axis=0)
    pad = 2 * total
    spot = lax.broadcasted_iota(jnp.int32, (1, pad), 1)
    exp_sums = jnp.where(spot < total, added, 1.0)
    losses = weights * (jnp.log(exp_sums) - pltpu.roll(added, total, 1))
    mean = jnp.sum(losses, axis=1, keepdims=True) / jnp.maximum(
        jnp.sum(weights, axis=1, keepdims=True), 1.0
    )
    start = (s * nf + f) * tok
    mine_out = pltpu.roll(losses, lax.rem(pad - start, pad), 1)
    out[...] = jnp.where(spot < tok, mine_out, mean)[0, 0:out.shape[0]]

    mark("drain")
    for way in (0, 1):
        for j in range(1, nf):
            going = has_up if way == 0 else has_down

            @pl.when(jnp.logical_and(going, held(way, j - 1)))
            def _():
                remote(
                    gathered.at[0], gathered.at[0], hid_send.at[way, j - 1], hid_recv.at[0, 0], f, m, 1 - s
                ).wait_send()
    swap.wait_send()
    near_swap.wait_send()
    far_sum.wait_send()
    if nm > 1:
        peers(near_mid, near_mp).wait_send()
    for way in (0, 1):
        for j in range(rest):
            going = jnp.logical_and(has_up if way == 0 else has_down, held(way, j))
            for zs, when in ((share(j + 1), late(way)), (whole_z, jnp.logical_not(late(way)))):
                @pl.when(jnp.logical_and(going, when))
                def _():
                    ref = res.at[s, 0, zs]
                    remote(
                        ref, ref, res_sem.at[4 + way * nf + j], res_recv.at[0], f, m, 1 - s
                    ).wait_send()

    res_in.wait_send()
    if halved and nm > 1:
        @pl.when(edge)
        def _():
            res_x.wait_send()

    info_in.wait_send()
    mom_in.wait_send()
    near_all = states.at[pl.ds(0, rest), 0, pl.ds(0, rest)]
    remote(near_all, near_all, near_send, near_recv.at[0], f, m, 1 - s).wait_send()
    for h in (0, 1):
        far_all = states.at[pl.ds(0, nf - h), 0, 0]
        remote(far_all, far_all, far_send, far_recv.at[0], f, m, 1 - s).wait_send()
    near_all = states.at[:, 0, pl.ds(0, rest)]
    remote(near_all, near_all, near_fwd.at[nf], near_fwd.at[0], f, m, 1 - s).wait_send()
    sum_in.wait_send()
    mark(None)


def finish(tok, row, losses, mean):
    losses[...] = row[0:tok]
    mean[...] = row[tok:tok + 1]


def on_device(
    nf, nm, hidden, residual, down_packed, down_scale, post_gain, final_gain, embed_packed, embed_scale,
    targets, loss_mask,
):
    tok, width_d = residual.shape
    rows, cols = down_packed.shape
    vocab, packed = embed_packed.shape
    half = rows // 2
    half_k = half * PLANES
    n = nf * nm * 2
    total = tok * 2 * nf
    rest = nf - 1
    groups = half_k // GROUP
    pieces = next(c for c in PIECES if groups % c == 0 and half_k // c % 256 == 0 or c == 1)
    piece = half_k // pieces
    width = 256 if piece % 256 == 0 else GROUP
    vm = pl.BlockSpec(memory_space=pltpu.VMEM)
    hbm = pl.BlockSpec(memory_space=pltpu.HBM)
    dma = pltpu.SemaphoreType.DMA
    bf16, f32, i32 = jnp.bfloat16, jnp.float32, jnp.int32
    row = pl.pallas_call(
        functools.partial(kernel, nf, nm),
        out_shape=jax.ShapeDtypeStruct((128,), f32),
        in_specs=[hbm] * 10,
        out_specs=vm,
        scratch_shapes=[
            pltpu.VMEM(hidden.shape, bf16),
            pltpu.VMEM(residual.shape, bf16),
            pltpu.VMEM((half, cols), i32),
            pltpu.VMEM(down_scale.shape, bf16),
            pltpu.VMEM((width_d,), f32),
            pltpu.VMEM((width_d,), f32),
            pltpu.VMEM((packed, vocab), i32),
            pltpu.VMEM((embed_scale.shape[1], vocab), bf16),
            pltpu.SMEM((tok,), i32),
            pltpu.SMEM((tok,), i32),
            pltpu.VMEM(down_scale.shape, f32),
            pltpu.VMEM((embed_scale.shape[1], vocab), f32),
            pltpu.VMEM((nf, 1, cols), f32),
            pltpu.VMEM((nf, 1, cols), f32),
            pltpu.VMEM((half_k, cols), bf16),
            pltpu.VMEM((width_d, vocab), bf16),
            pltpu.VMEM((width, width), bf16),
            pltpu.VMEM((2, pieces, tok, piece), bf16),
            pltpu.VMEM((nf, pieces, 2, tok, piece), bf16),
            pltpu.VMEM((2, rest * tok, cols), f32),
            pltpu.VMEM((rest * tok, cols), f32),
            pltpu.VMEM((rest * tok, cols), f32),
            pltpu.VMEM((nm, rest * tok, cols), f32),
            pltpu.VMEM((2, tok, cols), f32),
            pltpu.VMEM((2 * nm, tok, cols), f32),
            pltpu.VMEM((nf, tok, cols), f32),
            pltpu.VMEM((2, nf, nf, tok, cols), bf16),
            pltpu.VMEM((nf, 2, nf, tok, cols), bf16),
            pltpu.VMEM((2 * nf, 1, 256), f32),
            pltpu.VMEM((nf, total, cols), f32),
            pltpu.VMEM((total, vocab), f32),
            pltpu.VMEM((total, 128), f32),
            pltpu.VMEM((1, 128), i32),
            pltpu.VMEM((2 * nf, 1, 128), i32),
            pltpu.VMEM((n, 1, 2 * total), f32),
            dma((10,)),
            dma((2, max(nf - 1, 1))), dma((nf, pieces)),
            dma((2,)), dma((2,)), dma((2,)), dma((2,)),
            dma((4 + 2 * nf,)), dma((nf,)), dma((2,)),
            dma, dma((nf,)), dma, dma((nf,)), dma((nf + 1,)),
            dma((2,)), dma((2,)),
        ],
        compiler_params=pltpu.CompilerParams(
            collective_id=0, has_side_effects=True, vmem_limit_bytes=60 * 1024 * 1024
        ),
    )(
        hidden, residual, down_packed, down_scale, post_gain, final_gain,
        embed_packed.T, embed_scale.T, targets, loss_mask,
    )
    return pl.pallas_call(
        functools.partial(finish, tok),
        out_shape=(jax.ShapeDtypeStruct((tok,), f32), jax.ShapeDtypeStruct((1,), f32)),
        in_specs=[vm],
        out_specs=(vm, vm),
    )(row)


def solution(mesh):
    nf, nm = mesh.shape["fsdp"], mesh.shape["mp"]
    return jax.shard_map(
        functools.partial(on_device, nf, nm),
        mesh=mesh,
        in_specs=(
            P(("groups", "fsdp", "sub"), "mp"),
            P(("groups", "fsdp", "sub"), None),
            P("mp", "fsdp"),
            P("mp", "fsdp"),
            P(),
            P(),
            P(("fsdp", "mp", "sub"), None),
            P(("fsdp", "mp", "sub"), None),
            P(("groups", "fsdp", "sub")),
            P(("groups", "fsdp", "sub")),
        ),
        out_specs=(P(("groups", "fsdp", "sub")), P("groups")),
        check_vma=False,
    )
```

```python
import functools

import jax
import jax.numpy as jnp
from jax import lax
from jax.experimental import pallas as pl
from jax.experimental.pallas import tpu as pltpu
from jax.sharding import PartitionSpec as P

EPS = 1e-06
CAP = 30.0
MESH = pl.DeviceIdType.MESH
PLANES = 8
GROUP = 128
PIECES = (9, 8, 6, 4, 3, 2, 1)


def remote(src, dst, send, recv, f, m, s):
    return pltpu.make_async_remote_copy(
        src_ref=src,
        dst_ref=dst,
        send_sem=send,
        recv_sem=recv,
        device_id={"fsdp": f, "mp": m, "sub": s},
        device_id_type=MESH,
    )


def mark(name):
    pass


def kernel(
    nf, nm, hidden_hbm, residual_hbm, words_hbm, scale_hbm, post_hbm, final_hbm, embed_hbm, embed_scale_hbm,
    targets_hbm, mask_hbm,
    out,
    hidden, residual, words, scale, post_gain, final_gain, embed_words, embed_scale, targets, mask,
    scale_f, embed_f, post_z, final_z, weight, embed, perm, sorted_own, gathered,
    near_own, near_in, near_part, near_mid, far_own, far_mid,
    ffn, res, states, moments, ratio, base_sum, power_sum, info, infos, sums,
    local_sem, hid_send, hid_recv, pair_sem, near_sem, near_mp, far_mp, res_sem, res_recv, info_sem,
    near_send, near_recv, far_send, far_recv, near_fwd, mom_sem, sum_sem,
):
    f, m, s = lax.axis_index("fsdp"), lax.axis_index("mp"), lax.axis_index("sub")
    n = nf * nm * 2
    me = (f * nm + m) * 2 + s
    tok = hidden.shape[0]
    half_rows, cols = words.shape
    half_k = half_rows * PLANES
    total = tok * 2 * nf
    width_d = nf * cols
    pieces, piece = gathered.shape[1], gathered.shape[4]
    groups = half_k // GROUP
    per = GROUP // PLANES
    rest = nf - 1
    low = f < nf - nf // 2
    far = jnp.where(low, nf - 1, 0)
    first = jnp.where(low, 0, 1)
    up, down = lax.rem(f + 1, nf), lax.rem(f + nf - 1, nf)
    has_up, has_down = f < nf - 1, f > 0
    inner = jnp.logical_and(has_up, has_down)

    def where_is(q):
        return q // (2 * nm), (q // 2) % nm, q % 2

    barrier = pltpu.get_barrier_semaphore()

    def greet(pf, pm, ps):
        pl.semaphore_signal(
            barrier, inc=1, device_id={"fsdp": pf, "mp": pm, "sub": ps}, device_id_type=MESH
        )

    @pl.when(has_up)
    def _():
        greet(up, m, 0)
        greet(up, m, 1)

    @pl.when(has_down)
    def _():
        greet(down, m, 0)
        greet(down, m, 1)

    greet(f, m, 1 - s)
    for d in range(1, nm):
        greet(f, lax.rem(m + d, nm), s)

    def load(i, src, dst):
        copy = pltpu.make_async_copy(src, dst, local_sem.at[i])
        copy.start()
        return copy

    load_hidden = load(0, hidden_hbm, hidden)
    load_residual = load(5, residual_hbm, residual)
    load_words = load(
        1, words_hbm.at[pl.ds(pl.multiple_of(s * half_rows, 8), half_rows)], words
    )
    load_scale = load(2, scale_hbm, scale)
    loads = [
        load(3, embed_hbm, embed_words), load(4, embed_scale_hbm, embed_scale),
        load(6, post_hbm, post_gain), load(7, final_hbm, final_gain),
        load(8, targets_hbm, targets), load(9, mask_hbm, mask),
    ]

    width = perm.shape[0]
    row = lax.broadcasted_iota(jnp.int32, (width, width), 0)
    col = lax.broadcasted_iota(jnp.int32, (width, width), 1)
    inside = jnp.bitwise_and(col, GROUP - 1)
    source = (col - inside) + jnp.bitwise_and(inside, per - 1) * PLANES + jnp.right_shift(inside, 4)
    perm[...] = jnp.where(row == source, 1.0, 0.0).astype(jnp.bfloat16)

    mark("hidden_wait")
    load_hidden.wait()
    mark("permute")
    own = hidden[...].astype(jnp.float32)
    spans = 2 * half_k // width
    stacked = jnp.concatenate(
        [own[:, c * width:(c + 1) * width] for c in range(spans)], axis=0
    ).astype(jnp.bfloat16)
    ordered = jnp.dot(stacked, perm[...], preferred_element_type=jnp.float32)
    for c in range(spans):
        h, at = c * width // half_k, c * width % half_k
        sorted_own[h, at // piece, :, at % piece:at % piece + width] = ordered[
            c * tok:(c + 1) * tok
        ].astype(jnp.bfloat16)

    mark("barrier")
    count = 1 + (nm - 1) + 2 * has_up.astype(jnp.int32) + 2 * has_down.astype(jnp.int32)
    pl.semaphore_wait(barrier, count)
    mark("send1")

    def first_hop(way, i):
        target = up if way == 0 else down
        for h in (0, 1):
            remote(
                sorted_own.at[h, i], gathered.at[f, i, s], hid_send.at[way, 0], hid_recv.at[f, i],
                target, m, h,
            ).start()

    def block_at(way, j):
        return lax.rem(f - j + nf, nf) if way == 0 else lax.rem(f + j, nf)

    def held(way, j):
        return f >= j if way == 0 else f + j <= nf - 1

    def arrive(b, i):
        remote(
            gathered.at[b, i], gathered.at[b, i], hid_send.at[0, 0], hid_recv.at[b, i], f, m, 1 - s
        ).wait_recv()

    def pass_on(j, i):
        for way in (0, 1):
            b = block_at(way, j)
            target = up if way == 0 else down

            @pl.when(jnp.logical_and(inner, held(way, j)))
            def _():
                arrive(b, i)
                remote(
                    gathered.at[b, i], gathered.at[b, i], hid_send.at[way, j], hid_recv.at[b, i],
                    target, m, s,
                ).start()

    for i in range(pieces):
        @pl.when(has_up)
        def _():
            first_hop(0, i)

        @pl.when(has_down)
        def _():
            first_hop(1, i)

    swap = remote(
        sorted_own.at[1 - s], gathered.at[f, :, s], pair_sem.at[0], pair_sem.at[1], f, m, 1 - s
    )
    swap.start()
    gathered[f, :, s] = sorted_own[s]
    load_residual.wait()
    own_res = residual[...].astype(jnp.float32)
    for z in range(nf):
        res[s, f, z] = own_res[:, z * cols:(z + 1) * cols].astype(jnp.bfloat16)

    halved = nf > 2 and nf % nm == 0
    span_z = nf // nm if halved else nf
    whole_z = pl.ds(0, nf)
    part_z = pl.ds(m * span_z, span_z) if halved else whole_z

    def share(d):
        return part_z if d < rest else whole_z

    def late(way):
        return jnp.logical_and(inner, (f == nf - 2) if way == 0 else (f == 1))

    def res_arrive(b, zs):
        ref = res.at[s, b, zs]
        remote(ref, ref, res_sem.at[0], res_recv.at[b], f, m, 1 - s).wait_recv()

    def res_send(way, j, when, zs=pl.ds(0, nf)):
        b = block_at(way, j)
        going = has_up if way == 0 else has_down

        @pl.when(jnp.logical_and(jnp.logical_and(going, held(way, j)), when))
        def _():
            if j > 0:
                res_arrive(b, pl.ds(0, nf))
            ref = res.at[s, b, zs]
            remote(
                ref, ref, res_sem.at[4 + way * nf + j], res_recv.at[b], up if way == 0 else down, m, s
            ).start()

    def res_pair(b, zs):
        ref = res.at[s, b, zs]
        remote(ref, ref, res_sem.at[0], res_sem.at[1], f, m, 1 - s).start()

    for way in (0, 1):
        res_send(way, 0, jnp.logical_not(inner))
    res_pair(f, pl.ds(0, nf))

    mark("deq")
    load_scale.wait()
    scale_f[...] = scale[...].astype(jnp.float32)
    load_words.wait()

    def dequant(g, carry):
        w = words[pl.ds(pl.multiple_of(g * per, per), per), :]
        sc = scale_f[pl.ds(s * groups + g, 1), :]
        for k in range(PLANES):
            code = jnp.right_shift(jnp.left_shift(w, 28 - 4 * k), 28) if k < 7 else jnp.right_shift(w, 28)
            weight[pl.ds(pl.multiple_of(g * GROUP + k * per, per), per), :] = (
                code.astype(jnp.float32) * sc
            ).astype(jnp.bfloat16)
        return carry

    each = groups // pieces
    lag = min(3, pieces)
    for i in range(pieces):
        lax.fori_loop(i * each, (i + 1) * each, dequant, 0)
        if i >= lag and nf > 2:
            pass_on(1, i - lag)

    mark("deqE")
    for copy in loads:
        copy.wait()
    embed_f[...] = embed_scale[...].astype(jnp.float32)
    packed, vocab = embed_words.shape
    span = packed * PLANES // embed_f.shape[0]
    step = 32
    blocks = packed // step

    def dequant_embed(i, carry):
        w = embed_words[pl.ds(pl.multiple_of(i * step, step), step), :]
        for k in range(PLANES):
            code = jnp.right_shift(jnp.left_shift(w, 28 - 4 * k), 28) if k < 7 else jnp.right_shift(w, 28)
            sc = embed_f[pl.ds((k * packed + i * step) // span, 1), :]
            embed[pl.ds(pl.multiple_of(k * packed + i * step, step), step), :] = (
                code.astype(jnp.float32) * sc
            ).astype(jnp.bfloat16)
        return carry

    def dequant_some(part, parts):
        lax.fori_loop(part * blocks // parts, (part + 1) * blocks // parts, dequant_embed, 0)

    for part in range(lag):
        dequant_some(part, lag)
        if nf > 2:
            pass_on(1, pieces - lag + part)
    for j in range(2, nf - 2):
        for i in range(pieces):
            pass_on(j, i)

    mark("prep")
    post_row, final_row = post_gain[...].reshape(1, width_d), final_gain[...].reshape(1, width_d)
    for z in range(nf):
        post_z[z] = post_row[:, z * cols:(z + 1) * cols]
        final_z[z] = final_row[:, z * cols:(z + 1) * cols]
    side = lax.broadcasted_iota(jnp.int32, (1, 128), 1)
    entry = jnp.zeros((1, 128), jnp.int32)
    for i in range(tok):
        entry = jnp.where(side == i, targets[i], jnp.where(side == 64 + i, mask[i], entry))
    info[...] = entry
    infos[s * nf + f] = entry

    for j in range(rest):
        for way in (0, 1):
            res_send(way, j, jnp.logical_and(inner, jnp.logical_not(late(way))))

    mark("near_mm")
    swap.wait_recv()
    edge = jnp.logical_not(inner)
    near_acc = jnp.zeros((rest * 2 * tok, cols), jnp.float32)
    for i in range(pieces):
        if nf > 3:
            pass_on(nf - 2, i)
        for b in range(nf):
            @pl.when(jnp.logical_and(edge, jnp.logical_and(f != b, far != b)))
            def _():
                arrive(b, i)

        lhs = gathered[pl.ds(first, rest), i].astype(jnp.float32).reshape(
            rest * 2 * tok, piece
        ).astype(jnp.bfloat16)
        near_acc = near_acc + jnp.dot(
            lhs, weight[i * piece:(i + 1) * piece], preferred_element_type=jnp.float32
        )
    for b in range(rest):
        for h in (0, 1):
            at = (2 * b + h) * tok
            near_own[h, b * tok:(b + 1) * tok] = near_acc[at:at + tok]
    near_swap = remote(
        near_own.at[1 - s], near_in, near_sem.at[0], near_sem.at[1], f, m, 1 - s
    )
    near_swap.start()
    for way in (0, 1):
        res_send(way, 0, late(way), share(1))

    def to_peers(part, mid, sems):
        for d in range(1, nm):
            remote(
                part, mid.at[m], sems.at[0], sems.at[1], f, lax.rem(m + d, nm), s
            ).start()

    def peers(mid, sems):
        ref = mid.at[pl.ds(0, nm - 1)]
        return remote(ref, ref, sems.at[0], sems.at[1], f, m, 1 - s)

    def gather_peers(part, mid, sems):
        if nm > 1:
            peers(mid, sems).wait_recv()
        full = part[...]
        for d in range(1, nm):
            full = full + mid[lax.rem(m + d, nm)]
        return full

    def nearer(d):
        return jnp.where(low, lax.rem(f + d, nf), lax.rem(f + nf - d, nf))

    def early_sends():
        spot = infos.at[s * nf + f]
        for d in range(1, nf):
            for h in (0, 1):
                remote(info, spot, info_sem.at[0], info_sem.at[1], lax.rem(f + d, nf), m, h).start()
        remote(info, spot, info_sem.at[0], info_sem.at[1], f, m, 1 - s).start()

    gains = post_z[f] * final_z[f]
    near_at = pl.ds(first, rest)

    def near_to(z, pf, ps, send, recv):
        return remote(
            states.at[z, s, near_at], states.at[z, s, near_at], send, recv, pf, m, ps
        )

    def near_span(z):
        return pl.ds(jnp.where(z < nf - nf // 2, 0, 1), rest)

    def far_spot(z):
        return jnp.where(z < nf - nf // 2, nf - 1, 0)

    def near_states():
        near_ffn = gather_peers(near_part, near_mid, near_mp)
        ffn[pl.ds(first, rest)] = near_ffn.reshape(rest, tok, cols)
        states[f, s, near_at] = (near_ffn * gains).reshape(rest, tok, cols).astype(jnp.bfloat16)
        for d in range(rest, 0, -1):
            near_to(f, nearer(d), s, near_send, near_recv.at[f]).start()
        near_to(f, f, 1 - s, near_fwd.at[nf], near_fwd.at[f]).start()

    mark("far_mm")
    far_acc = jnp.zeros((2 * tok, cols), jnp.float32)
    reduce_at, send_at = min(1, pieces - 1), min(6, pieces - 1)
    for i in range(pieces):
        if i == pieces - 1 and i > reduce_at:
            near_states()
        @pl.when(edge)
        def _():
            arrive(far, i)

        lhs = gathered[far, i].astype(jnp.float32).reshape(2 * tok, piece).astype(jnp.bfloat16)
        far_acc = far_acc + jnp.dot(
            lhs, weight[i * piece:(i + 1) * piece], preferred_element_type=jnp.float32
        )
        if i == reduce_at:
            near_swap.wait_recv()
            near_part[...] = near_own[s] + near_in[...]
            to_peers(near_part, near_mid, near_mp)
            if pieces - 1 <= reduce_at:
                near_states()
        if i == send_at:
            early_sends()
        for j in range(1, rest):
            if i == min(4 + j, pieces - 1):
                for way in (0, 1):
                    res_send(way, j, late(way), share(j + 1))
    for h in (0, 1):
        far_own[h] = far_acc[h * tok:(h + 1) * tok]
    mark("far_swap")
    slot = far_mid.at[2 * m + s]
    for d in range(1, nm):
        for h in (0, 1):
            remote(
                far_own.at[h], slot, far_mp.at[0], far_mp.at[1], f, lax.rem(m + d, nm), h
            ).start()
    remote(far_own.at[1 - s], slot, far_mp.at[0], far_mp.at[1], f, m, 1 - s).start()
    far_mid[2 * m + s] = far_own[s]

    mark("res_x")

    def res_hand(d):
        b = nearer(d)

        @pl.when(edge)
        def _():
            res_arrive(b, share(d))
            ref = res.at[s, b, part_z]
            if halved and d < rest:
                for e in range(1, nm):
                    remote(
                        ref, ref, res_sem.at[2], res_sem.at[3], f, lax.rem(m + e, nm), s
                    ).start()
            res_pair(b, share(d))

        @pl.when(inner)
        def _():
            res_pair(b, pl.ds(0, nf))

    for d in range(1, rest):
        res_hand(d)
    mark("far_mp")
    far_all = far_mid.at[pl.ds(0, 2 * nm - 1)]
    far_sum = remote(far_all, far_all, far_mp.at[0], far_mp.at[1], f, m, 1 - s)
    far_sum.wait_recv()
    far_ffn = jnp.sum(far_mid[...], axis=0)
    ffn[far] = far_ffn
    states[f, s, far] = (far_ffn * gains).astype(jnp.bfloat16)

    mark("moments")
    mine = nf * tok
    y = ffn[...].reshape(mine, cols)
    g = y * post_z[f]
    lane = lax.broadcasted_iota(jnp.int32, (mine, 128), 1)

    def row_sum(v):
        return jnp.sum(v, axis=1, keepdims=True)

    def tall(v):
        extra = 128 - v.shape[0]
        return v if extra == 0 else jnp.concatenate([v, jnp.zeros((extra, 128), jnp.float32)], axis=0)

    both_rows = jnp.transpose(tall(jnp.where(lane < 1, row_sum(y * y), row_sum(g * g))))
    moments[2 * f + s] = jnp.concatenate([both_rows[0:1], both_rows[1:2]], axis=1)
    mine_mom = moments.at[2 * f + s]
    for d in range(rest, 0, -1):
        for h in (0, 1):
            remote(mine_mom, mine_mom, mom_sem.at[0], mom_sem.at[1], nearer(d), m, h).start()
    remote(mine_mom, mine_mom, mom_sem.at[0], mom_sem.at[1], f, m, 1 - s).start()

    mine_far = states.at[f, s, far]
    for d in range(rest, 0, -1):
        for h in (0, 1):
            remote(mine_far, mine_far, far_send, far_recv.at[f], nearer(d), m, h).start()
    remote(mine_far, mine_far, far_send, far_recv.at[f], f, m, 1 - s).start()

    def same(z, span, sems, recv):
        ref = states.at[z, s, span]
        return remote(ref, ref, sems, recv, f, m, 1 - s)

    def other(z, span, sems, recv):
        ref = states.at[z, 1 - s, span]
        return remote(ref, ref, sems, recv, f, m, 1 - s)

    def hand_near(d):
        z = nearer(d)
        same(z, near_span(z), near_send, near_recv.at[z]).wait_recv()
        same(z, near_span(z), near_fwd.at[nf], near_fwd.at[z]).start()

    def crossed(d):
        z = nearer(d)
        return row_sum(states[z].astype(jnp.float32).reshape(total, cols) * ratio[z])

    def product(d):
        z = nearer(d)
        other(z, near_span(z), near_fwd.at[nf], near_fwd.at[z]).wait_recv()
        ref = states.at[z, 1 - s, far_spot(z)] if d == 0 else states.at[z, :, far_spot(z)]
        remote(ref, ref, far_send, far_recv.at[z], f, m, 1 - s).wait_recv()
        wide = states[z].astype(jnp.float32).reshape(total, cols)
        return jnp.dot(
            wide.astype(jnp.bfloat16), embed[pl.ds(pl.multiple_of(z * cols, 32), cols), :],
            preferred_element_type=jnp.float32,
        )

    mark("info")
    info_all = infos.at[pl.ds(0, 2 * nf - 1)]
    info_in = remote(info_all, info_all, info_sem.at[0], info_sem.at[1], f, m, 1 - s)
    info_in.wait_recv()
    turned = jnp.transpose(tall(infos[...].astype(jnp.float32).reshape(2 * nf, 128)))
    wanted = jnp.concatenate([turned[0:tok, e:e + 1] for e in range(2 * nf)], axis=0).astype(jnp.int32)
    counted = jnp.concatenate([turned[64:64 + tok, e:e + 1] for e in range(2 * nf)], axis=0)
    weights = jnp.transpose(
        jnp.concatenate(
            [jnp.broadcast_to(counted, (total, 128)), jnp.zeros((total, 128), jnp.float32)], axis=0
        )
    )[0:1, :]

    mark("res_wait")
    res_hand(rest)
    rest_ref = res.at[s, pl.ds(0, max(rest - 1, 1)), pl.ds(0, max(nf - span_z, 1))]
    res_x = remote(rest_ref, rest_ref, res_sem.at[2], res_sem.at[3], f, m, 1 - s)
    if halved and nm > 1:
        @pl.when(edge)
        def _():
            res_x.wait_recv()
            for d in range(1, rest):
                for e in range(1, nm):
                    res_pair(nearer(d), pl.ds(lax.rem(m + e, nm) * span_z, span_z))

    res_in = remote(res.at[1 - s], res.at[1 - s], res_sem.at[0], res_sem.at[1], f, m, 1 - s)
    def residual_product():
        res_in.wait_recv()
        power = jnp.zeros((total, 1), jnp.float32)
        base = jnp.zeros((2 * total, vocab), jnp.float32)
        for z in range(nf):
            rz = res[:, :, z].astype(jnp.float32).reshape(total, cols)
            power = power + row_sum(rz * rz)
            ratio[z] = rz / final_z[z]
            rf = rz * final_z[z]
            high = rf.astype(jnp.bfloat16)
            low_part = (rf - high.astype(jnp.float32)).astype(jnp.bfloat16)
            base = base + jnp.dot(
                jnp.concatenate([high, low_part], axis=0), embed[z * cols:(z + 1) * cols],
                preferred_element_type=jnp.float32,
            )
        base_sum[...] = base[0:total] + base[total:]
        power_sum[...] = jnp.broadcast_to(power, (total, 128))

    mark("logits0a")

    @pl.when(inner)
    def _():
        residual_product()

    mark("near_fwd1")
    for d in range(1, rest):
        hand_near(d)
    hand_near(rest)
    mark("product0")
    main = product(0)
    mark("logits0b")

    @pl.when(edge)
    def _():
        residual_product()

    base, power = base_sum[...], power_sum[:, 0:1]
    cross = crossed(0)

    mark("logits1")
    for d in range(1, rest):
        main, cross = main + product(d), cross + crossed(d)
    mark("last")
    mom_all = moments.at[pl.ds(0, 2 * nf - 1)]
    mom_in = remote(mom_all, mom_all, mom_sem.at[0], mom_sem.at[1], f, m, 1 - s)
    mom_in.wait_recv()
    halves = [
        functools.reduce(jnp.add, [moments[2 * z + h] for z in range(nf)]) for h in (0, 1)
    ]
    turned = jnp.transpose(tall(jnp.concatenate(
        [half[:, k:k + 128] for k in (0, 128) for half in halves], axis=0
    )))

    def column(q):
        return jnp.concatenate([turned[0:mine, 2 * q:2 * q + 1], turned[0:mine, 2 * q + 1:2 * q + 2]], axis=0)

    inv = lax.rsqrt(column(0) / width_d + EPS)
    square = power + inv * inv * column(1)
    mark("logits2")
    main, cross = main + product(rest), cross + crossed(rest)
    inv2 = lax.rsqrt((square + 2.0 * inv * cross) / width_d + EPS)
    logits = (base + main * inv) * inv2
    capped = CAP * jnp.tanh(logits / CAP)
    ids = me * vocab + lax.broadcasted_iota(jnp.int32, (total, vocab), 1)
    hits = wanted == ids
    e = jnp.sum(jnp.exp(capped), axis=1, keepdims=True)
    t = jnp.sum(jnp.where(hits, capped, 0.0), axis=1, keepdims=True)
    both = jnp.concatenate(
        [jnp.broadcast_to(e, (total, 128)), jnp.broadcast_to(t, (total, 128))], axis=0
    )
    sums[me] = jnp.transpose(both)[0:1, :]
    mark("sums")
    for d in range(1, n):
        pf, pm, ps = where_is(lax.rem(me + d, n))
        remote(sums.at[me], sums.at[me], sum_sem.at[0], sum_sem.at[1], pf, pm, ps).start()
    sum_all = sums.at[pl.ds(0, n - 1)]
    sum_in = remote(sum_all, sum_all, sum_sem.at[0], sum_sem.at[1], f, m, 1 - s)
    sum_in.wait_recv()
    mark("final")
    added = jnp.sum(sums[...], axis=0)
    pad = 2 * total
    spot = lax.broadcasted_iota(jnp.int32, (1, pad), 1)
    exp_sums = jnp.where(spot < total, added, 1.0)
    losses = weights * (jnp.log(exp_sums) - pltpu.roll(added, total, 1))
    mean = jnp.sum(losses, axis=1, keepdims=True) / jnp.maximum(
        jnp.sum(weights, axis=1, keepdims=True), 1.0
    )
    start = (s * nf + f) * tok
    mine_out = pltpu.roll(losses, lax.rem(pad - start, pad), 1)
    out[...] = jnp.where(spot < tok, mine_out, mean)[0, 0:out.shape[0]]

    mark("drain")
    for way in (0, 1):
        for j in range(1, nf):
            going = has_up if way == 0 else has_down

            @pl.when(jnp.logical_and(going, held(way, j - 1)))
            def _():
                remote(
                    gathered.at[0], gathered.at[0], hid_send.at[way, j - 1], hid_recv.at[0, 0], f, m, 1 - s
                ).wait_send()
    swap.wait_send()
    near_swap.wait_send()
    far_sum.wait_send()
    if nm > 1:
        peers(near_mid, near_mp).wait_send()
    for way in (0, 1):
        for j in range(rest):
            going = jnp.logical_and(has_up if way == 0 else has_down, held(way, j))
            for zs, when in ((share(j + 1), late(way)), (whole_z, jnp.logical_not(late(way)))):
                @pl.when(jnp.logical_and(going, when))
                def _():
                    ref = res.at[s, 0, zs]
                    remote(
                        ref, ref, res_sem.at[4 + way * nf + j], res_recv.at[0], f, m, 1 - s
                    ).wait_send()

    res_in.wait_send()
    if halved and nm > 1:
        @pl.when(edge)
        def _():
            res_x.wait_send()

    info_in.wait_send()
    mom_in.wait_send()
    near_all = states.at[pl.ds(0, rest), 0, pl.ds(0, rest)]
    remote(near_all, near_all, near_send, near_recv.at[0], f, m, 1 - s).wait_send()
    for h in (0, 1):
        far_all = states.at[pl.ds(0, nf - h), 0, 0]
        remote(far_all, far_all, far_send, far_recv.at[0], f, m, 1 - s).wait_send()
    near_all = states.at[:, 0, pl.ds(0, rest)]
    remote(near_all, near_all, near_fwd.at[nf], near_fwd.at[0], f, m, 1 - s).wait_send()
    sum_in.wait_send()
    mark(None)


def finish(tok, row, losses, mean):
    losses[...] = row[0:tok]
    mean[...] = row[tok:tok + 1]


def on_device(
    nf, nm, hidden, residual, down_packed, down_scale, post_gain, final_gain, embed_packed, embed_scale,
    targets, loss_mask,
):
    tok, width_d = residual.shape
    rows, cols = down_packed.shape
    vocab, packed = embed_packed.shape
    half = rows // 2
    half_k = half * PLANES
    n = nf * nm * 2
    total = tok * 2 * nf
    rest = nf - 1
    groups = half_k // GROUP
    pieces = next(c for c in PIECES if groups % c == 0 and half_k // c % 256 == 0 or c == 1)
    piece = half_k // pieces
    width = 256 if piece % 256 == 0 else GROUP
    vm = pl.BlockSpec(memory_space=pltpu.VMEM)
    hbm = pl.BlockSpec(memory_space=pltpu.HBM)
    dma = pltpu.SemaphoreType.DMA
    bf16, f32, i32 = jnp.bfloat16, jnp.float32, jnp.int32
    row = pl.pallas_call(
        functools.partial(kernel, nf, nm),
        out_shape=jax.ShapeDtypeStruct((128,), f32),
        in_specs=[hbm] * 10,
        out_specs=vm,
        scratch_shapes=[
            pltpu.VMEM(hidden.shape, bf16),
            pltpu.VMEM(residual.shape, bf16),
            pltpu.VMEM((half, cols), i32),
            pltpu.VMEM(down_scale.shape, bf16),
            pltpu.VMEM((width_d,), f32),
            pltpu.VMEM((width_d,), f32),
            pltpu.VMEM((packed, vocab), i32),
            pltpu.VMEM((embed_scale.shape[1], vocab), bf16),
            pltpu.SMEM((tok,), i32),
            pltpu.SMEM((tok,), i32),
            pltpu.VMEM(down_scale.shape, f32),
            pltpu.VMEM((embed_scale.shape[1], vocab), f32),
            pltpu.VMEM((nf, 1, cols), f32),
            pltpu.VMEM((nf, 1, cols), f32),
            pltpu.VMEM((half_k, cols), bf16),
            pltpu.VMEM((width_d, vocab), bf16),
            pltpu.VMEM((width, width), bf16),
            pltpu.VMEM((2, pieces, tok, piece), bf16),
            pltpu.VMEM((nf, pieces, 2, tok, piece), bf16),
            pltpu.VMEM((2, rest * tok, cols), f32),
            pltpu.VMEM((rest * tok, cols), f32),
            pltpu.VMEM((rest * tok, cols), f32),
            pltpu.VMEM((nm, rest * tok, cols), f32),
            pltpu.VMEM((2, tok, cols), f32),
            pltpu.VMEM((2 * nm, tok, cols), f32),
            pltpu.VMEM((nf, tok, cols), f32),
            pltpu.VMEM((2, nf, nf, tok, cols), bf16),
            pltpu.VMEM((nf, 2, nf, tok, cols), bf16),
            pltpu.VMEM((2 * nf, 1, 256), f32),
            pltpu.VMEM((nf, total, cols), f32),
            pltpu.VMEM((total, vocab), f32),
            pltpu.VMEM((total, 128), f32),
            pltpu.VMEM((1, 128), i32),
            pltpu.VMEM((2 * nf, 1, 128), i32),
            pltpu.VMEM((n, 1, 2 * total), f32),
            dma((10,)),
            dma((2, max(nf - 1, 1))), dma((nf, pieces)),
            dma((2,)), dma((2,)), dma((2,)), dma((2,)),
            dma((4 + 2 * nf,)), dma((nf,)), dma((2,)),
            dma, dma((nf,)), dma, dma((nf,)), dma((nf + 1,)),
            dma((2,)), dma((2,)),
        ],
        compiler_params=pltpu.CompilerParams(
            collective_id=0, has_side_effects=True, vmem_limit_bytes=60 * 1024 * 1024
        ),
    )(
        hidden, residual, down_packed, down_scale, post_gain, final_gain,
        embed_packed.T, embed_scale.T, targets, loss_mask,
    )
    return pl.pallas_call(
        functools.partial(finish, tok),
        out_shape=(jax.ShapeDtypeStruct((tok,), f32), jax.ShapeDtypeStruct((1,), f32)),
        in_specs=[vm],
        out_specs=(vm, vm),
    )(row)


def solution(mesh):
    nf, nm = mesh.shape["fsdp"], mesh.shape["mp"]
    return jax.shard_map(
        functools.partial(on_device, nf, nm),
        mesh=mesh,
        in_specs=(
            P(("groups", "fsdp", "sub"), "mp"),
            P(("groups", "fsdp", "sub"), None),
            P("mp", "fsdp"),
            P("mp", "fsdp"),
            P(),
            P(),
            P(("fsdp", "mp", "sub"), None),
            P(("fsdp", "mp", "sub"), None),
            P(("groups", "fsdp", "sub")),
            P(("groups", "fsdp", "sub")),
        ),
        out_specs=(P(("groups", "fsdp", "sub")), P("groups")),
        check_vma=False,
    )
```
